256 devices in a mesh: dom: 4 (over x_lo, core), orient: 64 (over x_hi, y, z).
Axes of the slice: x: 4 (x_hi: 2, x_lo: 2; x = x_hi * 2 + x_lo), y: 4, z: 8, core: 2. Of those that a mesh axis runs over, the one named last changes fastest.
Arguments:
- particles: bfloat16 [2048, 2, 8192], P(('dom', 'orient')), may hold values from -48 to 48
- templates: bfloat16 [16384, 2, 8192], P('orient'), may hold values from -6 to 6
- tilt_low: int32 [2048], P(('dom', 'orient')), may hold values from 0 to 23
- tilt_high: int32 [2048], P(('dom', 'orient')), may hold values from 40 to 63
Outputs:
- updated: float32 [16384, 2, 8192], P('orient', None, 'dom')
- log_evidence: float32 [2048], P('dom')
The draws below stay inside these ranges and needn't reach their ends.
All inputs are finite; a program needn't handle non-finite values.
Results may differ from the reference program's by a relative error of at most 0.0045.
Values may be sent and summed in bfloat16 or wider, within the bound.
A program may use at most 192 MiB of HBM per device.

```python
import math
import jax
import jax.numpy as jnp
from jax import lax

K = 8192
NBIN = 64
R_DEV = 256
P_GRP = 512
R = 16384
P_SIZE = 2048
N_DOM = 4


def template_values(key):
    template_key = jax.random.fold_in(key, 11)
    return jnp.clip(jax.random.normal(template_key, (R, 2, K), jnp.float32), -6.0, 6.0)


def draw_templates(key, part):
    return template_values(key).astype(jnp.bfloat16)


def draw_particles(key, part):
    noise_key = jax.random.fold_in(key, 23)
    noise_values = jnp.clip(jax.random.normal(noise_key, (P_SIZE, 2, K), jnp.float32), -6.0, 6.0)
    factor = 0.5 + 60.0 / math.sqrt(K)
    chosen_refs = jax.random.randint(jax.random.fold_in(key, 29), (P_SIZE,), 0, R)
    aligned = factor * template_values(key).astype(jnp.bfloat16).astype(jnp.float32)[chosen_refs]
    picked_rows = jnp.arange(P_SIZE) % 16 == 0
    noise_values = jnp.where(picked_rows[:, None, None], aligned, noise_values)
    noise_values = jnp.clip(noise_values, -48.0, 48.0)
    return noise_values.astype(jnp.bfloat16)


def with_ends(entries, rng, smallest, high):
    place = [jax.random.randint(jax.random.fold_in(rng, axis), (), 0, length) for axis, length in enumerate(entries.shape)]
    widest = entries.shape.index(max(entries.shape))
    beside = place[:widest] + [(place[widest] + 1) % entries.shape[widest]] + place[widest + 1:]
    return entries.at[tuple(place)].set(smallest).at[tuple(beside)].set(high)


def setup_inputs(seed: int = 0) -> dict:
    streams_of = jax.random.split(jax.random.key(seed), 5)
    return {
        "particles": draw_particles(jax.random.fold_in(streams_of[4], 71), 0),
        "templates": draw_templates(jax.random.fold_in(streams_of[4], 71), 0),
        "tilt_low": with_ends(jax.random.randint(streams_of[2], (P_SIZE,), 0, 24), jax.random.fold_in(streams_of[2], 1), 0, 23).astype(jnp.int32),
        "tilt_high": with_ends(jax.random.randint(streams_of[3], (P_SIZE,), 40, 64), jax.random.fold_in(streams_of[3], 1), 40, 63).astype(jnp.int32),
    }


def bin_index(band_size):
    return jnp.arange(band_size, dtype=jnp.int32) * 37 % NBIN

def reference(particles, templates, tilt_low, tilt_high):
    inverse_temp = 3.0 / math.sqrt(K)
    binned = bin_index(K)
    observed = ((tilt_low[:, None] <= binned[None, :]) & (binned[None, :] < tilt_high[:, None])).astype(jnp.bfloat16)
    masked = particles * observed[:, None, :]
    flat_rows = masked.reshape(P_SIZE, 2 * K)
    residue_mask = observed[:, :NBIN].astype(jnp.float32)
    blocks = R // R_DEV
    template_blocks = templates.reshape(blocks, R_DEV, 2, K)

    def score_block(template_block):
        template_flat = template_block.reshape(R_DEV, 2 * K)
        correlation = lax.dot_general(flat_rows, template_flat, (((1,), (1,)), ((), ())), preferred_element_type=jnp.float32)
        real_part = template_block[:, 0, :].astype(jnp.float32)
        imag_part = template_block[:, 1, :].astype(jnp.float32)
        power = real_part * real_part + imag_part * imag_part
        residue_power = lax.optimization_barrier(jnp.sum(power.reshape(R_DEV, K // NBIN, NBIN), axis=1))
        penalty = jnp.dot(residue_mask, residue_power.T, precision=lax.Precision.HIGHEST)
        return inverse_temp * (correlation - 0.5 * penalty)
    scores = lax.map(score_block, template_blocks)
    scores = jnp.transpose(scores, (1, 0, 2)).reshape(P_SIZE, R)
    peak_score = lax.optimization_barrier(jnp.max(scores, axis=1))
    total_mass = lax.optimization_barrier(jnp.sum(jnp.exp(scores - peak_score[:, None]), axis=1))
    log_evidence = peak_score + jnp.log(total_mass)
    weights = jnp.exp(scores - log_evidence[:, None]).astype(jnp.bfloat16)
    weight_blocks = jnp.transpose(weights.reshape(P_SIZE, blocks, R_DEV), (1, 0, 2))

    def update_block(inputs):
        weight_block, template_block = inputs
        numerator = jnp.zeros((R_DEV, 2 * K), jnp.float32)
        denominator = jnp.zeros((R_DEV, K), jnp.float32)
        for group_id in range(N_DOM):
            lower = group_id * P_GRP
            group_weights = weight_block[lower:lower + P_GRP]
            part_num = lax.dot_general(group_weights, flat_rows[lower:lower + P_GRP], (((0,), (0,)), ((), ())), preferred_element_type=jnp.float32)
            part_den = lax.dot_general(group_weights, observed[lower:lower + P_GRP], (((0,), (0,)), ((), ())), preferred_element_type=jnp.float32)
            part_num = lax.optimization_barrier(part_num.astype(jnp.bfloat16))
            part_den = lax.optimization_barrier(part_den.astype(jnp.bfloat16))
            numerator = numerator + part_num.astype(jnp.float32)
            denominator = denominator + part_den.astype(jnp.float32)
        numerator = numerator.reshape(R_DEV, 2, K)
        return (numerator + template_block.astype(jnp.float32)) / (denominator[:, None, :] + 1.0)
    updated = lax.map(update_block, (weight_blocks, template_blocks)).reshape(R, 2, K)
    return (updated, log_evidence)
```

```python
import functools
import math

import jax
import jax.numpy as jnp
from jax import lax
from jax.experimental import pallas as pl
from jax.experimental.pallas import tpu as pltpu
from jax.sharding import PartitionSpec as P

NBIN = 64
NX, NY, NZ, ND = 2, 4, 8, 4
LANES = 128
RING = (0, 7, 1, 6, 2, 5, 3, 4)
BW = {"x": 23.3, "y+": 46.6, "y-": 46.6, "z+": 46.6, "z-": 46.6}
LATENCY = 2.0


def moved(unit, link):
    x, z, y = unit
    if link == "x":
        return 1 - x, z, y
    step = -1 if link[1] == "+" else 1
    return (x, (z + step) % NZ, y) if link[0] == "z" else (x, z, (y + step) % NY)


def plan(cols, first_a, second_a, x_cols):
    sends = []

    def add(link, unit, part, lo, hi, rank):
        sends.append(
            dict(link=link, unit=unit, part=part, lo=lo, hi=hi, rank=rank, lands=moved(unit, link))
        )

    add("x", (0, 0, 0), "F", 0, cols, 0)
    for x in (0, 1):
        cut, end = (first_a, cols) if x == 0 else (second_a, cols - x_cols)
        plus = x == 0
        add("y+", (x, 0, 0), "A", 0, cut, 0)
        add("y-", (x, 0, 0), "A", 0, cut, 0)
        add(*(("y+", (x, 0, 3)) if plus else ("y-", (x, 0, 1))), "A", 0, cut, 0)
        for k in range(4):
            if k < 3 or plus:
                add("z+", (x, -k % NZ, 0), "B", cut, end, 1)
            if k < 3 or not plus:
                add("z-", (x, k, 0), "B", cut, end, 1)
        for k in range(4):
            for y in (0, 3, 1, 2):
                if k < 3 or y in (0, 3):
                    add("z+", (x, -k % NZ, y), "A", 0, cut, 2)
                if k < 3 or y in (1, 2):
                    add("z-", (x, k, y), "A", 0, cut, 2)
        for n, z in enumerate(RING):
            add("y+", (x, z, 0), "B", cut, end, 2)
            add("y-", (x, z, 0), "B", cut, end, 2)
            add(*(("y+", (x, z, 3)) if n % 2 == 0 else ("y-", (x, z, 1))), "B", cut, end, 2)
        if x == 0 and x_cols:
            for z in RING:
                for y in (0, 3, 1, 2):
                    if (z, y) != (0, 0):
                        add("x", (0, z, y), "X", cols - x_cols, cols, 3)
    for number, s in enumerate(sends):
        s["id"] = number
    arrives = {(s["lands"], s["part"]): s["id"] for s in sends}
    for s in sends:
        part = "B" if s["part"] == "X" else s["part"]
        own = {(0, 0, 0): None, (1, 0, 0): 0}
        s["needs"] = own[s["unit"]] if s["unit"] in own else arrives[s["unit"], part]

    free, landed, left, events = dict.fromkeys(BW, 0.0), {None: 0.0}, list(sends), []
    while left:
        able = [s for s in left if s["needs"] in landed]
        key = lambda s: (
            max(landed[s["needs"]], free[s["link"]]), s["unit"][0], s["rank"], s["id"]
        )
        s = min(able, key=key)
        start = max(landed[s["needs"]], free[s["link"]])
        free[s["link"]] = start + (s["hi"] - s["lo"]) * 8.192 / BW[s["link"]]
        landed[s["id"]] = free[s["link"]] + LATENCY
        events.append(s)
        left.remove(s)
    when, latest = {}, dict.fromkeys(BW, 0.0)
    for s in events:
        latest[s["link"]] = max(latest[s["link"]], landed[s["needs"]])
        when[s["id"]] = latest[s["link"]]
    batches = []
    for x in (0, 1):
        for z in range(NZ):
            wanted = [
                arrives[(x, z, y), part]
                for y in range(NY)
                for part in "FABX"
                if ((x, z, y), part) in arrives
            ]
            batches.append((max(landed[w] for w in wanted), x, z, wanted))
    batches.sort()
    order = sorted(events, key=lambda s: when[s["id"]])
    segments, at = [], 0
    for done, _, _, wanted in batches:
        stop = at
        while stop < len(order) and when[order[stop]["id"]] <= done:
            stop += 1
        segments.append((order[at:stop], wanted))
        at = stop
    assert at == len(order)
    return sends, segments, [(x, z) for _, x, z, _ in batches]


def table(values, index):
    total = jnp.int32(0)
    for n, v in enumerate(values):
        if v:
            total = total + jnp.where(index == n, v, 0)
    return total


def em_kernel(
    schedule, temp, block, temps, out, lz_out,
    rows, scores, parts, weights, evid, stat, stat_z, stat_q, power, inverse, local_sem,
    send_sem, recv_sem, ps_send, ps_recv, zs_send, zs_recv, qs_send, qs_recv,
    w_send, w_recv, l_send, l_recv,
):
    sends, segments, batches = schedule
    dom, orient = lax.axis_index("dom"), lax.axis_index("orient")
    x0, y0, z0 = orient // (NY * NZ), (orient // NZ) % NY, orient % NZ
    q0 = x0 * NY + y0
    width = temps.shape[1]
    refs = temps.shape[0]

    def at(x, y, z):
        return {"orient": (x * NY + y) * NZ + z}

    def at_q(q):
        return {"orient": q * NZ + z0}

    target = {
        "x": at(1 - x0, y0, z0),
        "y+": at(x0, (y0 + 1) % NY, z0),
        "y-": at(x0, (y0 + NY - 1) % NY, z0),
        "z+": at(x0, y0, (z0 + 1) % NZ),
        "z-": at(x0, y0, (z0 + NZ - 1) % NZ),
    }
    z_peer = [at(x0, y0, (z0 + k) % NZ) for k in range(NZ)]
    q_peer = [at_q((q0 + k) % (NX * NY)) for k in range(NX * NY)]
    d_peer = [{"dom": (dom + k) % ND} for k in range(ND)]
    chip_peer = {"dom": dom + 1 - 2 * (dom % 2)}
    side_peer = {"dom": (dom + 2) % ND}
    chip_dom = dom + 1 - 2 * (dom % 2)
    side_dom = (dom + 2) % ND

    barrier = pltpu.get_barrier_semaphore()
    greeted = z_peer[1:] + q_peer[1:] + d_peer[1:]
    for peer in greeted:
        pl.semaphore_signal(barrier, inc=1, device_id=peer, device_id_type=pl.DeviceIdType.MESH)
    pl.semaphore_wait(barrier, len(greeted))

    z_at = [((z0 + k) % NZ % ND) * 512 + ((z0 + k) % NZ // ND) * 128 for k in range(NZ)]
    y_at = [((y0 + k) % NY) * 32 for k in range(NY)]
    x_at = [x0 * 256, (1 - x0) * 256]

    def unit_rows(unit):
        x, z, y = unit
        return pl.ds(pl.multiple_of(x_at[x] + z_at[z] + y_at[y], 32), 32)

    def remote(src, dst, ssem, rsem, peer):
        return pltpu.make_async_remote_copy(
            src_ref=src, dst_ref=dst, send_sem=ssem, recv_sem=rsem,
            device_id=peer, device_id_type=pl.DeviceIdType.MESH,
        )

    def copy_of(s, unit):
        columns = pl.ds(s["lo"] * LANES, (s["hi"] - s["lo"]) * LANES)
        place = rows.at[unit_rows(unit), columns]
        src = block.at[:, columns] if unit == (0, 0, 0) else place
        return remote(
            src, place, send_sem.at[s["id"]], recv_sem.at[s["id"]], target[s["link"]]
        )

    own = pltpu.make_async_copy(block, rows.at[unit_rows((0, 0, 0)), :], local_sem)
    own.start()

    heard = set()

    def hear(number):
        if number is not None and number not in heard:
            heard.add(number)
            copy_of(sends[number], sends[number]["lands"]).wait_recv()

    def partial_copy(pos):
        owner, part = pos // ND, pos % ND
        rel = (dom - owner + ND) % ND - 1
        return remote(
            scores.at[pos], parts.at[jnp.maximum(rel, 0), part], ps_send.at[pos],
            ps_recv.at[jnp.maximum(rel, 0), part], {"dom": owner},
        )

    def phase_body(phase, carry):
        for n, (issue, wanted) in enumerate(segments):

            @pl.when(phase == n)
            def _(n=n, issue=issue, wanted=wanted):
                for s in issue:
                    hear(s["needs"])
                    copy_of(s, s["unit"]).start()
                for w in wanted:
                    hear(w)
                if n == 0:
                    own.wait()
                    total = jnp.zeros((refs, LANES), jnp.float32)
                    for c in range(width // LANES):
                        piece = temps[:, c * LANES : (c + 1) * LANES].astype(jnp.float32)
                        total = total + piece * piece
                    total = 0.5 * total
                    for c in range(3):
                        head = total.astype(jnp.bfloat16)
                        power[c] = head
                        total = total - head.astype(jnp.float32)

        bx = table([b[0] for b in batches], phase)
        bz = (z0 + table([b[1] for b in batches], phase)) % NZ
        bx = (x0 + bx) % NX
        pos = (bz % ND) * ND + bx * 2 + bz // ND
        here = pl.ds(pl.multiple_of(pos * LANES, LANES), LANES)
        nt = (((1,), (1,)), ((), ()))
        mask = rows[here, width : width + LANES]
        penalty = lax.dot_general(power[2], mask, nt, preferred_element_type=jnp.float32)
        for c in (1, 0):
            penalty = penalty + lax.dot_general(
                power[c], mask, nt, preferred_element_type=jnp.float32
            )
        corr = lax.dot_general(
            temps[...], rows[here, :width], nt, preferred_element_type=jnp.float32
        )
        scores[pos] = corr - penalty

        @pl.when(pos // ND != dom)
        def _():
            partial_copy(pos).start()

        return carry

    lax.fori_loop(0, len(segments), phase_body, 0)

    peaks, masses = [], []
    for part in range(ND):
        mine = dom * ND + part
        total = scores[mine]
        for rel in range(ND - 1):
            remote(
                scores.at[mine], parts.at[rel, part], ps_send.at[mine], ps_recv.at[rel, part],
                d_peer[1],
            ).wait_recv()
            total = total + parts[rel, part]
        total = total * temp
        parts[0, part] = total
        peak = jnp.max(total, axis=0, keepdims=True)
        peaks.append(peak)
        masses.append(jnp.sum(jnp.exp(total - peak), axis=0, keepdims=True))
    stat[...] = jnp.concatenate(peaks + masses, axis=0)

    def merge(slots, index, peers, ssem, rsem):
        copies = [
            remote(stat, slots.at[index], ssem.at[k], rsem.at[k], peers[k])
            for k in range(1, len(peers))
        ]
        for c in copies:
            c.start()
        own_stat = stat[...]
        slots[index] = own_stat
        for k, c in enumerate(copies):
            src = (index + 2 * len(peers) - (k + 1)) % len(peers)
            remote(stat, slots.at[src], ssem.at[k + 1], rsem.at[k + 1], peers[k + 1]).wait_recv()
        both = slots[...]
        peak = jnp.max(both[:, :ND], axis=0)
        mass = jnp.sum(both[:, ND:] * jnp.exp(both[:, :ND] - peak[None]), axis=0)
        for c in copies:
            c.wait_send()
        return peak, mass

    peak, mass = merge(stat_z, z0, z_peer, zs_send, zs_recv)
    stat[...] = jnp.concatenate([peak, mass], axis=0)
    peak, mass = merge(stat_q, q0, q_peer, qs_send, qs_recv)
    log_evidence = peak + jnp.log(mass)
    evid[dom] = jnp.concatenate([log_evidence, log_evidence], axis=0)
    my_cols = pl.multiple_of(dom * 512, 512)
    for part in range(ND):
        w = jnp.exp(parts[0, part] - log_evidence[part : part + 1])
        weights[:, pl.ds(my_cols + part * LANES, LANES)] = w.astype(jnp.bfloat16)

    def w_copy(n, owner, peer):
        ref = weights.at[:, pl.ds(pl.multiple_of(owner * 512, 512), 512)]
        return remote(ref, ref, w_send.at[n], w_recv.at[n], peer)

    def l_copy(k, owner):
        return remote(evid.at[owner], evid.at[owner], l_send.at[k], l_recv.at[k], d_peer[k])

    w_copy(0, dom, side_peer).start()
    w_copy(1, dom, chip_peer).start()
    for k in range(1, ND):
        l_copy(k, dom).start()
    w_copy(0, side_dom, side_peer).wait_recv()
    w_copy(2, side_dom, chip_peer).start()
    w_copy(1, chip_dom, chip_peer).wait_recv()
    w_copy(2, (chip_dom + 2) % ND, chip_peer).wait_recv()

    den = jnp.dot(
        weights[...], rows[:, width : width + LANES], preferred_element_type=jnp.float32
    )
    inverse[...] = 1.0 / (den + 1.0)

    def tile(j, carry):
        columns = pl.ds(pl.multiple_of(j * 256, 256), 256)
        num = jnp.dot(weights[...], rows[:, columns], preferred_element_type=jnp.float32)
        scale = inverse[...]
        out[:, columns] = (num + temps[:, columns].astype(jnp.float32)) * jnp.concatenate(
            [scale, scale], axis=1
        )
        return carry

    lax.fori_loop(0, width // 256, tile, 0)

    for k in range(1, ND):
        l_copy(k, (dom + ND - k) % ND).wait_recv()
    lz_out[...] = evid[...]
    for k in range(1, ND):
        l_copy(k, dom).wait_send()
    w_copy(0, dom, side_peer).wait_send()
    w_copy(1, dom, chip_peer).wait_send()
    w_copy(2, side_dom, chip_peer).wait_send()

    def drain(pos, carry):
        @pl.when(pos // ND != dom)
        def _():
            partial_copy(pos).wait_send()

        return carry

    lax.fori_loop(0, ND * ND, drain, 0)
    for s in sends:
        copy_of(s, s["unit"]).wait_send()


def on_device(particles, templates, tilt_low, tilt_high):
    local, _, band = particles.shape
    refs = templates.shape[0]
    quarter = band // ND
    width = 2 * quarter
    temp = 3.0 / math.sqrt(band)
    bins = jnp.arange(LANES, dtype=jnp.int32) * 37 % NBIN
    observed = (tilt_low[:, None] <= bins[None, :]) & (bins[None, :] < tilt_high[:, None])
    observed = observed.astype(jnp.bfloat16)
    masked = particles * jnp.tile(observed, (1, band // LANES))[:, None, :]
    split = jnp.transpose(masked.reshape(local, 2, ND, quarter), (2, 0, 1, 3))
    split = split.reshape(ND, local, width)
    split = jnp.concatenate(
        [split, jnp.broadcast_to(observed[None], (ND, local, LANES))], axis=2
    )
    block = lax.all_to_all(split, "dom", split_axis=0, concat_axis=0, tiled=True)
    block = block.reshape(ND * local, width + LANES)
    start = lax.axis_index("dom") * quarter
    temps = lax.dynamic_slice_in_dim(templates, start, quarter, 2).reshape(refs, width)

    schedule = plan((width + LANES) // LANES, 13, 11, 6)
    count = len(schedule[0])
    dma = pltpu.SemaphoreType.DMA
    updated, evidence = pl.pallas_call(
        functools.partial(em_kernel, schedule, temp),
        out_shape=(
            jax.ShapeDtypeStruct((refs, width), jnp.float32),
            jax.ShapeDtypeStruct((ND, 8, LANES), jnp.float32),
        ),
        in_specs=[pl.BlockSpec(memory_space=pltpu.VMEM)] * 2,
        out_specs=(pl.BlockSpec(memory_space=pltpu.VMEM),) * 2,
        scratch_shapes=[
            pltpu.VMEM((NX * NY * NZ * ND * local, width + LANES), jnp.bfloat16),
            pltpu.VMEM((ND * ND, refs, LANES), jnp.float32),
            pltpu.VMEM((ND - 1, ND, refs, LANES), jnp.float32),
            pltpu.VMEM((refs, NX * NY * NZ * ND * local), jnp.bfloat16),
            pltpu.VMEM((ND, 8, LANES), jnp.float32),
            pltpu.VMEM((8, LANES), jnp.float32),
            pltpu.VMEM((NZ, 8, LANES), jnp.float32),
            pltpu.VMEM((NX * NY, 8, LANES), jnp.float32),
            pltpu.VMEM((3, refs, LANES), jnp.bfloat16),
            pltpu.VMEM((refs, LANES), jnp.float32),
            dma(()),
            dma((count,)),
            dma((count,)),
            dma((ND * ND,)),
            dma((ND - 1, ND)),
            dma((NZ,)),
            dma((NZ,)),
            dma((NX * NY,)),
            dma((NX * NY,)),
            dma((3,)),
            dma((3,)),
            dma((ND,)),
            dma((ND,)),
        ],
        compiler_params=pltpu.CompilerParams(
            collective_id=0, has_side_effects=True, vmem_limit_bytes=60 * 1024 * 1024
        ),
    )(block, temps)
    evidence = evidence[:, :ND].reshape(ND, NX, NZ // ND, NY, ND, local)
    evidence = lax.dynamic_index_in_dim(evidence, lax.axis_index("dom"), 4, keepdims=False)
    evidence = jnp.transpose(evidence, (1, 3, 2, 0, 4)).reshape(-1)
    return updated.reshape(refs, 2, quarter), evidence


def solution(mesh):
    in_specs = (
        P(("dom", "orient"), None, None),
        P("orient", None, None),
        P(("dom", "orient")),
        P(("dom", "orient")),
    )
    out_specs = (P("orient", None, "dom"), P("dom"))
    return jax.shard_map(
        on_device, mesh=mesh, in_specs=in_specs, out_specs=out_specs, check_vma=False
    )
```

```python
import functools
import math

import jax
import jax.numpy as jnp
from jax import lax
from jax.experimental import pallas as pl
from jax.experimental.pallas import tpu as pltpu
from jax.sharding import PartitionSpec as P

NBIN = 64
NX, NY, NZ, ND = 2, 4, 8, 4
LANES = 128
RING = (0, 7, 1, 6, 2, 5, 3, 4)
BW = {"x": 46.6, "y+": 46.6, "y-": 46.6, "z+": 46.6, "z-": 46.6}
LATENCY = 2.0


def moved(unit, link):
    x, z, y = unit
    if link == "x":
        return 1 - x, z, y
    step = -1 if link[1] == "+" else 1
    return (x, (z + step) % NZ, y) if link[0] == "z" else (x, z, (y + step) % NY)


def plan(cols, first_a, second_a, x_cols):
    sends = []

    def add(link, unit, part, lo, hi, rank):
        sends.append(
            dict(link=link, unit=unit, part=part, lo=lo, hi=hi, rank=rank, lands=moved(unit, link))
        )

    add("x", (0, 0, 0), "F", 0, cols, 0)
    for x in (0, 1):
        cut, end = (first_a, cols) if x == 0 else (second_a, cols - x_cols)
        plus = x == 0
        add("y+", (x, 0, 0), "A", 0, cut, 0)
        add("y-", (x, 0, 0), "A", 0, cut, 0)
        add(*(("y+", (x, 0, 3)) if plus else ("y-", (x, 0, 1))), "A", 0, cut, 0)
        for k in range(4):
            if k < 3 or plus:
                add("z+", (x, -k % NZ, 0), "B", cut, end, 1)
            if k < 3 or not plus:
                add("z-", (x, k, 0), "B", cut, end, 1)
        for k in range(4):
            for y in (0, 3, 1, 2):
                if k < 3 or y in (0, 3):
                    add("z+", (x, -k % NZ, y), "A", 0, cut, 2)
                if k < 3 or y in (1, 2):
                    add("z-", (x, k, y), "A", 0, cut, 2)
        for n, z in enumerate(RING):
            add("y+", (x, z, 0), "B", cut, end, 2)
            add("y-", (x, z, 0), "B", cut, end, 2)
            add(*(("y+", (x, z, 3)) if n % 2 == 0 else ("y-", (x, z, 1))), "B", cut, end, 2)
        if x == 0 and x_cols:
            for z in RING:
                for y in (0, 3, 1, 2):
                    if (z, y) != (0, 0):
                        add("x", (0, z, y), "X", cols - x_cols, cols, 3)
    for number, s in enumerate(sends):
        s["id"] = number
    arrives = {(s["lands"], s["part"]): s["id"] for s in sends}
    for s in sends:
        part = "B" if s["part"] == "X" else s["part"]
        own = {(0, 0, 0): None, (1, 0, 0): 0}
        s["needs"] = own[s["unit"]] if s["unit"] in own else arrives[s["unit"], part]

    free, landed, left, events = dict.fromkeys(BW, 0.0), {None: 0.0}, list(sends), []
    while left:
        able = [s for s in left if s["needs"] in landed]
        key = lambda s: (
            max(landed[s["needs"]], free[s["link"]]), s["unit"][0], s["rank"], s["id"]
        )
        s = min(able, key=key)
        start = max(landed[s["needs"]], free[s["link"]])
        free[s["link"]] = start + (s["hi"] - s["lo"]) * 8.192 / BW[s["link"]]
        landed[s["id"]] = free[s["link"]] + LATENCY
        events.append(s)
        left.remove(s)
    when, latest = {}, dict.fromkeys(BW, 0.0)
    for s in events:
        latest[s["link"]] = max(latest[s["link"]], landed[s["needs"]])
        when[s["id"]] = latest[s["link"]]
    batches = []
    for x in (0, 1):
        for z in range(NZ):
            wanted = [
                arrives[(x, z, y), part]
                for y in range(NY)
                for part in "FABX"
                if ((x, z, y), part) in arrives
            ]
            batches.append((max(landed[w] for w in wanted), x, z, wanted))
    batches.sort()
    order = sorted(events, key=lambda s: when[s["id"]])
    segments, at = [], 0
    for done, _, _, wanted in batches:
        stop = at
        while stop < len(order) and when[order[stop]["id"]] <= done:
            stop += 1
        segments.append((order[at:stop], wanted))
        at = stop
    assert at == len(order)
    return sends, segments, [(x, z) for _, x, z, _ in batches]


def table(values, index):
    total = jnp.int32(0)
    for n, v in enumerate(values):
        if v:
            total = total + jnp.where(index == n, v, 0)
    return total


def em_kernel(
    schedule, temp, split, templates, rows_out, temps_out, weights, lz_out,
    pairs, temps, rows, scores, parts, evid, stat, stat_z, stat_q, power,
    local_sem, load_sem, temps_sem, rows_sem, a_send, a_recv,
    send_sem, recv_sem, ps_send, ps_recv, zs_send, zs_recv, qs_send, qs_recv,
    w_send, w_recv, l_send, l_recv,
):
    sends, segments, batches = schedule
    dom, orient = lax.axis_index("dom"), lax.axis_index("orient")
    x0, y0, z0 = orient // (NY * NZ), (orient // NZ) % NY, orient % NZ
    q0 = x0 * NY + y0
    refs, width = temps.shape

    def at(x, y, z):
        return {"orient": (x * NY + y) * NZ + z}

    def at_q(q):
        return {"orient": q * NZ + z0}

    target = {
        "x": at(1 - x0, y0, z0),
        "y+": at(x0, (y0 + 1) % NY, z0),
        "y-": at(x0, (y0 + NY - 1) % NY, z0),
        "z+": at(x0, y0, (z0 + 1) % NZ),
        "z-": at(x0, y0, (z0 + NZ - 1) % NZ),
    }
    z_peer = [at(x0, y0, (z0 + k) % NZ) for k in range(NZ)]
    q_peer = [at_q((q0 + k) % (NX * NY)) for k in range(NX * NY)]
    d_peer = [{"dom": (dom + k) % ND} for k in range(ND)]
    chip_peer = {"dom": dom + 1 - 2 * (dom % 2)}
    side_peer = {"dom": (dom + 2) % ND}
    chip_dom = dom + 1 - 2 * (dom % 2)
    side_dom = (dom + 2) % ND

    quarter = width // 2
    load = pltpu.make_async_copy(
        templates.at[:, :, pl.ds(pl.multiple_of(dom * quarter, quarter), quarter)],
        pairs,
        load_sem,
    )
    load.start()

    barrier = pltpu.get_barrier_semaphore()
    greeted = [z_peer[1], z_peer[NZ - 1], q_peer[NY]] + d_peer[1:]
    greeted += [target["y+"], target["y-"]]
    for peer in greeted:
        pl.semaphore_signal(barrier, inc=1, device_id=peer, device_id_type=pl.DeviceIdType.MESH)
    load.wait()

    def relayout(i, carry):
        r = pl.ds(pl.multiple_of(i * 16, 16), 16)
        for c in range(2):
            temps[r, c * quarter : (c + 1) * quarter] = pairs[r, c, :]
        return carry

    lax.fori_loop(0, refs // 16, relayout, 0)
    pl.semaphore_wait(barrier, len(greeted))

    z_at = [((z0 + k) % NZ % ND) * 512 + ((z0 + k) % NZ // ND) * 128 for k in range(NZ)]
    y_at = [((y0 + k) % NY) * 32 for k in range(NY)]
    x_at = [x0 * 256, (1 - x0) * 256]

    def unit_rows(unit):
        x, z, y = unit
        return pl.ds(pl.multiple_of(x_at[x] + z_at[z] + y_at[y], 32), 32)

    def remote(src, dst, ssem, rsem, peer):
        return pltpu.make_async_remote_copy(
            src_ref=src, dst_ref=dst, send_sem=ssem, recv_sem=rsem,
            device_id=peer, device_id_type=pl.DeviceIdType.MESH,
        )

    def copy_of(s, unit):
        columns = pl.ds(s["lo"] * LANES, (s["hi"] - s["lo"]) * LANES)
        place = rows.at[unit_rows(unit), columns]
        return remote(
            place, place, send_sem.at[s["id"]], recv_sem.at[s["id"]], target[s["link"]]
        )

    local = split.shape[0] // ND
    own_row = x_at[0] + z_at[0] + y_at[0]

    def a_copy(k, source, owner):
        return remote(
            split.at[pl.ds(pl.multiple_of(owner * local, local), local)],
            rows.at[pl.ds(pl.multiple_of(own_row + source * local, local), local)],
            a_send.at[k], a_recv.at[k], d_peer[k],
        )

    for k in (2, 3, 1):
        a_copy(k, dom, (dom + k) % ND).start()
    own = pltpu.make_async_copy(
        split.at[pl.ds(pl.multiple_of(dom * local, local), local)],
        rows.at[pl.ds(pl.multiple_of(own_row + dom * local, local), local)],
        local_sem,
    )
    own.start()
    own.wait()
    for k in (1, 2, 3):
        a_copy(k, (dom + ND - k) % ND, dom).wait_recv()

    heard = set()

    def hear(number):
        if number is not None and number not in heard:
            heard.add(number)
            copy_of(sends[number], sends[number]["lands"]).wait_recv()

    def partial_copy(pos):
        owner, part = pos // ND, pos % ND
        rel = (dom - owner + ND) % ND - 1
        return remote(
            scores.at[pos], parts.at[jnp.maximum(rel, 0), part], ps_send.at[pos],
            ps_recv.at[jnp.maximum(rel, 0), part], {"dom": owner},
        )

    def rows_copy(pos):
        here = pl.ds(pl.multiple_of(pos * LANES, LANES), LANES)
        return pltpu.make_async_copy(rows.at[here], rows_out.at[here], rows_sem.at[pos])

    temps_copy = pltpu.make_async_copy(temps, temps_out, temps_sem)
    temps_copy.start()

    def phase_body(phase, carry):
        for n, (issue, wanted) in enumerate(segments):

            @pl.when(phase == n)
            def _(n=n, issue=issue, wanted=wanted):
                for s in issue:
                    hear(s["needs"])
                    copy_of(s, s["unit"]).start()
                if n == 0:
                    total = jnp.zeros((refs, LANES), jnp.float32)
                    for c in range(width // LANES):
                        piece = temps[:, c * LANES : (c + 1) * LANES].astype(jnp.float32)
                        total = total + piece * piece
                    total = 0.5 * total
                    for c in range(3):
                        head = total.astype(jnp.bfloat16)
                        power[c] = head
                        total = total - head.astype(jnp.float32)
                for w in wanted:
                    hear(w)

        bx = table([b[0] for b in batches], phase)
        bz = (z0 + table([b[1] for b in batches], phase)) % NZ
        bx = (x0 + bx) % NX
        pos = (bz % ND) * ND + bx * 2 + bz // ND
        here = pl.ds(pl.multiple_of(pos * LANES, LANES), LANES)
        nt = (((1,), (1,)), ((), ()))
        mask = rows[here, width : width + LANES]
        penalty = lax.dot_general(power[2], mask, nt, preferred_element_type=jnp.float32)
        for c in (1, 0):
            penalty = penalty + lax.dot_general(
                power[c], mask, nt, preferred_element_type=jnp.float32
            )
        corr = lax.dot_general(
            temps[...], rows[here, :width], nt, preferred_element_type=jnp.float32
        )
        scores[pos] = corr - penalty

        @pl.when(pos // ND != dom)
        def _():
            partial_copy(pos).start()

        rows_copy(pos).start()
        return carry

    lax.fori_loop(0, len(segments), phase_body, 0)

    peaks, masses = [], []
    for part in range(ND):
        mine = dom * ND + part
        total = scores[mine]
        for rel in range(ND - 1):
            remote(
                scores.at[mine], parts.at[rel, part], ps_send.at[mine], ps_recv.at[rel, part],
                d_peer[1],
            ).wait_recv()
            total = total + parts[rel, part]
        total = total * temp
        parts[0, part] = total
        peak = jnp.max(total, axis=0, keepdims=True)
        peaks.append(peak)
        masses.append(jnp.sum(jnp.exp(total - peak), axis=0, keepdims=True))
    stat[...] = jnp.concatenate(peaks + masses, axis=0)

    def merge(slots, index, peers, ssem, rsem):
        copies = [
            remote(stat, slots.at[index], ssem.at[k], rsem.at[k], peers[k])
            for k in range(1, len(peers))
        ]
        for c in copies:
            c.start()
        own_stat = stat[...]
        slots[index] = own_stat
        for k, c in enumerate(copies):
            src = (index + 2 * len(peers) - (k + 1)) % len(peers)
            remote(stat, slots.at[src], ssem.at[k + 1], rsem.at[k + 1], peers[k + 1]).wait_recv()
        both = slots[...]
        peak = jnp.max(both[:, :ND], axis=0)
        mass = jnp.sum(both[:, ND:] * jnp.exp(both[:, :ND] - peak[None]), axis=0)
        for c in copies:
            c.wait_send()
        return peak, mass

    peak, mass = merge(stat_z, z0, z_peer, zs_send, zs_recv)
    stat[...] = jnp.concatenate([peak, mass], axis=0)
    peak, mass = merge(stat_q, q0, q_peer, qs_send, qs_recv)
    log_evidence = peak + jnp.log(mass)
    evid[dom] = jnp.concatenate([log_evidence, log_evidence], axis=0)
    my_cols = pl.multiple_of(dom * 512, 512)
    for part in range(ND):
        w = jnp.exp(parts[0, part] - log_evidence[part : part + 1])
        weights[:, pl.ds(my_cols + part * LANES, LANES)] = w.astype(jnp.bfloat16)

    def w_copy(n, owner, peer):
        ref = weights.at[:, pl.ds(pl.multiple_of(owner * 512, 512), 512)]
        return remote(ref, ref, w_send.at[n], w_recv.at[n], peer)

    def l_copy(k, owner):
        return remote(evid.at[owner], evid.at[owner], l_send.at[k], l_recv.at[k], d_peer[k])

    w_copy(0, dom, side_peer).start()
    w_copy(1, dom, chip_peer).start()
    for k in range(1, ND):
        l_copy(k, dom).start()
    w_copy(0, side_dom, side_peer).wait_recv()
    w_copy(2, side_dom, chip_peer).start()
    w_copy(1, chip_dom, chip_peer).wait_recv()
    w_copy(2, (chip_dom + 2) % ND, chip_peer).wait_recv()

    for k in range(1, ND):
        l_copy(k, (dom + ND - k) % ND).wait_recv()
    lz_out[...] = evid[...]
    temps_copy.wait()
    for k in range(1, ND):
        a_copy(k, dom, (dom + k) % ND).wait_send()
        l_copy(k, dom).wait_send()
    w_copy(0, dom, side_peer).wait_send()
    w_copy(1, dom, chip_peer).wait_send()
    w_copy(2, side_dom, chip_peer).wait_send()

    def drain(pos, carry):
        @pl.when(pos // ND != dom)
        def _():
            partial_copy(pos).wait_send()

        rows_copy(pos).wait()
        return carry

    lax.fori_loop(0, ND * ND, drain, 0)
    for s in sends:
        copy_of(s, s["unit"]).wait_send()


def update_kernel(weights, real, imag, mask, real_temps, imag_temps, out, inverse):
    @pl.when(pl.program_id(0) == 0)
    def _():
        den = jnp.dot(weights[...], mask[...], preferred_element_type=jnp.float32)
        inverse[...] = 1.0 / (den + 1.0)

    scale = jnp.concatenate([inverse[...]] * (real.shape[1] // LANES), axis=1)
    for c, (rows, temps) in enumerate(((real, real_temps), (imag, imag_temps))):
        num = jnp.dot(weights[...], rows[...], preferred_element_type=jnp.float32)
        out[:, c, :] = (num + temps[...].astype(jnp.float32)) * scale


def on_device(particles, templates, tilt_low, tilt_high):
    local, _, band = particles.shape
    refs = templates.shape[0]
    quarter = band // ND
    width = 2 * quarter
    temp = 3.0 / math.sqrt(band)
    bins = jnp.arange(LANES, dtype=jnp.int32) * 37 % NBIN
    observed = (tilt_low[:, None] <= bins[None, :]) & (bins[None, :] < tilt_high[:, None])
    observed = observed.astype(jnp.bfloat16)
    masked = particles * jnp.tile(observed, (1, band // LANES))[:, None, :]
    split = jnp.transpose(masked.reshape(local, 2, ND, quarter), (2, 0, 1, 3))
    split = split.reshape(ND, local, width)
    split = jnp.concatenate(
        [split, jnp.broadcast_to(observed[None], (ND, local, LANES))], axis=2
    )
    split = split.reshape(ND * local, width + LANES)
    schedule = plan((width + LANES) // LANES, 13, 9, 10)
    count = len(schedule[0])
    dma = pltpu.SemaphoreType.DMA
    total_rows = NX * NY * NZ * ND * local
    rows, temps, weights, evidence = pl.pallas_call(
        functools.partial(em_kernel, schedule, temp),
        out_shape=(
            jax.ShapeDtypeStruct((total_rows, width + LANES), jnp.bfloat16),
            jax.ShapeDtypeStruct((refs, width), jnp.bfloat16),
            jax.ShapeDtypeStruct((refs, total_rows), jnp.bfloat16),
            jax.ShapeDtypeStruct((ND, 8, LANES), jnp.float32),
        ),
        in_specs=[
            pl.BlockSpec(memory_space=pltpu.VMEM),
            pl.BlockSpec(memory_space=pl.ANY),
        ],
        out_specs=(pl.BlockSpec(memory_space=pl.ANY),) * 2
        + (pl.BlockSpec(memory_space=pltpu.VMEM),) * 2,
        scratch_shapes=[
            pltpu.VMEM((refs, 2, quarter), jnp.bfloat16),
            pltpu.VMEM((refs, width), jnp.bfloat16),
            pltpu.VMEM((total_rows, width + LANES), jnp.bfloat16),
            pltpu.VMEM((ND * ND, refs, LANES), jnp.float32),
            pltpu.VMEM((ND - 1, ND, refs, LANES), jnp.float32),
            pltpu.VMEM((ND, 8, LANES), jnp.float32),
            pltpu.VMEM((8, LANES), jnp.float32),
            pltpu.VMEM((NZ, 8, LANES), jnp.float32),
            pltpu.VMEM((NX * NY, 8, LANES), jnp.float32),
            pltpu.VMEM((3, refs, LANES), jnp.bfloat16),
            dma(()),
            dma(()),
            dma(()),
            dma((ND * ND,)),
            dma((ND,)),
            dma((ND,)),
            dma((count,)),
            dma((count,)),
            dma((ND * ND,)),
            dma((ND - 1, ND)),
            dma((NZ,)),
            dma((NZ,)),
            dma((NX * NY,)),
            dma((NX * NY,)),
            dma((3,)),
            dma((3,)),
            dma((ND,)),
            dma((ND,)),
        ],
        compiler_params=pltpu.CompilerParams(
            collective_id=0, has_side_effects=True, vmem_limit_bytes=60 * 1024 * 1024
        ),
    )(split, templates)
    tile = 256
    steps = quarter // tile
    updated = pl.pallas_call(
        update_kernel,
        out_shape=jax.ShapeDtypeStruct((refs, 2, quarter), jnp.float32),
        grid=(steps,),
        in_specs=[
            pl.BlockSpec((refs, total_rows), lambda j: (0, 0)),
            pl.BlockSpec((total_rows, tile), lambda j: (0, j)),
            pl.BlockSpec((total_rows, tile), lambda j: (0, j + steps)),
            pl.BlockSpec((total_rows, LANES), lambda j: (0, width // LANES)),
            pl.BlockSpec((refs, tile), lambda j: (0, j)),
            pl.BlockSpec((refs, tile), lambda j: (0, j + steps)),
        ],
        out_specs=pl.BlockSpec((refs, 2, tile), lambda j: (0, 0, j)),
        scratch_shapes=[pltpu.VMEM((refs, LANES), jnp.float32)],
        compiler_params=pltpu.CompilerParams(vmem_limit_bytes=60 * 1024 * 1024),
    )(weights, rows, rows, rows, temps, temps)
    evidence = evidence[:, :ND].reshape(ND, NX, NZ // ND, NY, ND, local)
    evidence = lax.dynamic_index_in_dim(evidence, lax.axis_index("dom"), 4, keepdims=False)
    evidence = jnp.transpose(evidence, (1, 3, 2, 0, 4)).reshape(-1)
    return updated, evidence


def solution(mesh):
    in_specs = (
        P(("dom", "orient"), None, None),
        P("orient", None, None),
        P(("dom", "orient")),
        P(("dom", "orient")),
    )
    out_specs = (P("orient", None, "dom"), P("dom"))
    return jax.shard_map(
        on_device, mesh=mesh, in_specs=in_specs, out_specs=out_specs, check_vma=False
    )
```

```python
import functools
import math

import jax
import jax.numpy as jnp
from jax import lax
from jax.experimental import pallas as pl
from jax.experimental.pallas import tpu as pltpu
from jax.sharding import PartitionSpec as P

NBIN = 64
NX, NY, NZ, ND, NH = 2, 4, 8, 4, 2
LANES = 128
RING = (0, 7, 1, 6, 2, 5, 3, 4)
LINKS = ("x", "y+", "y-", "z+", "z-")
LATENCY = 3.0
TILE = 0.0879
BATCH = 128
UNIT = 16
LOW_AT, HIGH_AT = 19, 83
MESH = pl.DeviceIdType.MESH


def moved(unit, link):
    h, x, z, y = unit
    if link == "x":
        return h, 1 - x, z, y
    step = -1 if link[1] == "+" else 1
    return (h, x, (z + step) % NZ, y) if link[0] == "z" else (h, x, z, (y + step) % NY)

def plan(cols, first_a, second_a, x_cols, chain=(5.0, 6.0, 6.0, 6.0), compute=0.95):
    sends = []
    def add(link, unit, part, lo, hi, rank):
        sends.append(dict(link=link, unit=unit, part=part, lo=lo, hi=hi, rank=rank, lands=moved(unit, link)))
    for h in range(NH):
        add("x", (h, 0, 0, 0), "F", 0, cols, 0)
        for x in (0, 1):
            cut, end = (first_a, cols) if x == 0 else (second_a, cols - x_cols)
            plus = (x + h) % 2 == 0
            add("y+", (h, x, 0, 0), "A", 0, cut, 0)
            add("y-", (h, x, 0, 0), "A", 0, cut, 0)
            link, y = ("y+", 3) if plus else ("y-", 1)
            add(link, (h, x, 0, y), "A", 0, cut, 0)
            for k in range(4):
                if k < 3 or plus:
                    add("z+", (h, x, -k % NZ, 0), "B", cut, end, 1)
                if k < 3 or not plus:
                    add("z-", (h, x, k, 0), "B", cut, end, 1)
            for k in range(4):
                for y in (0, 3, 1, 2):
                    if k < 3 or y in (0, 3):
                        add("z+", (h, x, -k % NZ, y), "A", 0, cut, 2)
                    if k < 3 or y in (1, 2):
                        add("z-", (h, x, k, y), "A", 0, cut, 2)
            for n, z in enumerate(RING):
                add("y+", (h, x, z, 0), "B", cut, end, 2)
                add("y-", (h, x, z, 0), "B", cut, end, 2)
                link, y = ("y+", 3) if n % 2 == 0 else ("y-", 1)
                add(link, (h, x, z, y), "B", cut, end, 2)
            if x == 0 and x_cols:
                for z in RING:
                    for y in (0, 3, 1, 2):
                        if (z, y) != (0, 0):
                            add("x", (h, 0, z, y), "X", cols - x_cols, cols, 3)
    for number, s in enumerate(sends):
        s["id"] = number
    arrives = {(s["lands"], s["part"]): s["id"] for s in sends}
    for s in sends:
        h, x, z, y = s["unit"]
        if (x, z, y) == (0, 0, 0):
            s["needs"] = None
        elif (x, z, y) == (1, 0, 0):
            s["needs"] = arrives[s["unit"], "F"]
        else:
            s["needs"] = arrives[s["unit"], "B" if s["part"] == "X" else s["part"]]
    forwarded = {s["needs"] for s in sends}
    groups = {}
    for s in sends:
        key = (s["part"], s["lands"][:3]) if s["id"] not in forwarded else s["id"]
        groups.setdefault(key, []).append(s)
    for sem, members in enumerate(groups.values()):
        assert len({(s["lo"], s["hi"]) for s in members}) == 1
        for s in members:
            s["sem"], s["group"] = sem, len(members)
    free, landed, left = dict.fromkeys(LINKS, 0.0), {None: 0.0}, list(sends)
    when = {}; latest = dict.fromkeys(LINKS, 0.0)
    while left:
        best = None
        for s in left:
            if s["needs"] in landed:
                key = (max(landed[s["needs"]], free[s["link"]]), s["unit"][:2], s["rank"], s["id"])
                if best is None or key < best[0]:
                    best = key, s
        (start, *_), s = best
        free[s["link"]] = start + (s["hi"] - s["lo"]) * TILE
        landed[s["id"]] = free[s["link"]] + LATENCY
        latest[s["link"]] = max(latest[s["link"]], landed[s["needs"]])
        when[s["id"]] = latest[s["link"]]
        left.remove(s)
    events = [(when[s["id"]], 0, s["id"], s) for s in sends]
    batches = []
    for h in range(NH):
        for z in range(NZ):
            wanted = [arrives[(h, x, z, y), p] for x in range(NX) for y in range(NY) for p in "FABX" if ((h, x, z, y), p) in arrives]
            batches.append((max(landed[w] for w in wanted), h, z, wanted))
    batches.sort()
    return sends, events, batches, free


def timeline(schedule, lags):
    sends, events, batches, _ = schedule
    first = max(b[0] for b in batches if b[1] == 0)
    steps = [(first + sum(lags[: n + 1]), 2, n, None) for n in range(len(lags))]
    marked = [(b[0], 1, n, b) for n, b in enumerate(batches)]
    segments, issue, order = [], [], []
    for _, kind, n, what in sorted(events + marked + steps, key=lambda e: e[:3]):
        if kind == 1:
            segments.append((issue, what[3]))
            order.append((what[1], what[2]))
            issue = []
        else:
            issue.append(what if kind == 0 else n)
    assert not any(isinstance(e, dict) for e in issue)
    return segments, order, issue


def table(values, index):
    total = jnp.int32(0)
    for n, v in enumerate(values):
        if v:
            total = total + jnp.where(index == n, v, 0)
    return total


def em_kernel(
    sends, line, temp, whole_particles, bounds, templates,
    rows, temps, edge, num, weights_1, inverse, evid,
    particles, split, pairs, masks, weights_0, scores, parts, stat_a, stat_b, stat_z, stat_q, power,
    local_sem, load_sem, a_send, a_recv, send_sem, recv_sem,
    ps_send, ps_recv, z_send, z_recv, q_send, q_recv, w_send, w_recv, l_send, l_recv,
):
    segments, batches, late = line
    dom, orient = lax.axis_index("dom"), lax.axis_index("orient")
    x0, y0, z0 = orient // (NY * NZ), (orient // NZ) % NY, orient % NZ
    q0 = x0 * NY + y0
    refs, width = temps.shape
    quarter = width // 2
    half = rows.shape[0] // NH
    share = half // ND

    def at(x, y, z):
        return {"orient": (x * NY + y) * NZ + z}

    z_peer = [at(x0, y0, (z0 + k) % NZ) for k in range(NZ)]
    q_peer = [{"orient": (q0 + k) % (NX * NY) * NZ + z0} for k in range(NX * NY)]
    d_peer = [{"dom": (dom + k) % ND} for k in range(ND)]
    target = {
        "x": q_peer[NY],
        "y+": at(x0, (y0 + 1) % NY, z0),
        "y-": at(x0, (y0 + NY - 1) % NY, z0),
        "z+": z_peer[1],
        "z-": z_peer[NZ - 1],
    }
    chip_dom = dom + 1 - 2 * (dom % 2)
    side_dom = (dom + 2) % ND
    chip_peer, side_peer = {"dom": chip_dom}, {"dom": side_dom}

    load = pltpu.make_async_copy(
        templates.at[:, :, pl.ds(pl.multiple_of(dom * quarter, quarter), quarter)],
        pairs,
        load_sem,
    )
    fetch = pltpu.make_async_copy(whole_particles, particles, local_sem)
    fetch.start()
    load.start()
    barrier = pltpu.get_barrier_semaphore()
    greeted = list(target.values()) + d_peer[1:]
    for peer in greeted:
        pl.semaphore_signal(barrier, inc=1, device_id=peer, device_id_type=MESH)

    def remote(src, dst, ssem, rsem, peer):
        return pltpu.make_async_remote_copy(
            src_ref=src, dst_ref=dst, send_sem=ssem, recv_sem=rsem,
            device_id=peer, device_id_type=MESH,
        )

    z_at = [
        ((z0 + k) % NZ % ND * 2 + (z0 + k) % NZ // ND) * BATCH for k in range(NZ)
    ]
    y_at = [(y0 + k) % NY * UNIT for k in range(NY)]
    x_at = [x0 * NY * UNIT, (1 - x0) * NY * UNIT]

    def unit_row(unit):
        h, x, z, y = unit
        return h * half + x_at[x] + z_at[z] + y_at[y]

    def relayout(i, carry):
        r = pl.ds(pl.multiple_of(i * 16, 16), 16)
        for c in range(2):
            temps[r, c * quarter : (c + 1) * quarter] = pairs[r, c, :]
        return carry

    local = particles.shape[0]
    item = lax.broadcasted_iota(jnp.int32, (local, 1), 0)
    low, high = jnp.zeros((local, 1), jnp.float32), jnp.zeros((local, 1), jnp.float32)
    for n in range(local):
        low = jnp.where(item == n, bounds[0, n].astype(jnp.float32), low)
        high = jnp.where(item == n, bounds[1, n].astype(jnp.float32), high)
    column = lax.broadcasted_iota(jnp.int32, (local, quarter), 1)
    bins = (column * 37 % NBIN).astype(jnp.float32)
    seen = (low <= bins) & (bins < high)
    stash = jnp.where(column == LOW_AT, low, jnp.where(column == HIGH_AT, high, 0.0))
    fetch.wait()
    for c in range(2):
        for d in range(ND):
            piece = particles[:, c, d * quarter : (d + 1) * quarter].astype(jnp.float32)
            piece = jnp.where(seen, piece, stash if c == 0 else 0.0)
            split[d * local : (d + 1) * local, c * quarter : (c + 1) * quarter] = piece.astype(
                jnp.bfloat16
            )
    pl.semaphore_wait(barrier, len(greeted))

    own_at = unit_row((0, 0, 0, 0))

    def split_at(owner):
        return split.at[pl.ds(pl.multiple_of(owner * local, local), local)]

    def own_rows(source):
        row = own_at + source // 2 * half + source % 2 * local
        return rows.at[pl.ds(pl.multiple_of(row, local), local)]

    def a_copy(k, source, owner):
        return remote(split_at(owner), own_rows(source), a_send.at[k], a_recv.at[k], d_peer[k])

    for k in (2, 3, 1):
        a_copy(k, dom, (dom + k) % ND).start()
    own = pltpu.make_async_copy(split_at(dom), own_rows(dom), local_sem)
    own.start()
    own.wait()
    for k in (1, 2, 3):
        a_copy(k, (dom + ND - k) % ND, dom).wait_recv()
    def copy_of(s, unit):
        columns = pl.ds(s["lo"] * LANES, (s["hi"] - s["lo"]) * LANES)
        place = rows.at[pl.ds(pl.multiple_of(unit_row(unit), UNIT), UNIT), columns]
        return remote(
            place, place, send_sem.at[unit[0]], recv_sem.at[s["sem"]], target[s["link"]]
        )

    heard = set()

    def hear(number):
        if number is None or sends[number]["sem"] in heard:
            return
        s = sends[number]
        heard.add(s["sem"])
        h, x, z, _ = s["lands"]
        columns = pl.ds(s["lo"] * LANES, (s["hi"] - s["lo"]) * LANES)
        if s["group"] == 1:
            row = unit_row(s["lands"])
        else:
            row = h * half + x_at[x] + z_at[z]
        place = rows.at[pl.ds(pl.multiple_of(row, UNIT), UNIT * s["group"]), columns]
        remote(
            place, place, send_sem.at[h], recv_sem.at[s["sem"]], target[s["link"]]
        ).wait_recv()

    def partial_copy(slot):
        owner, part = slot % (2 * ND) // 2, slot // (2 * ND) * 2 + slot % 2
        rel = jnp.maximum((dom - owner + ND) % ND - 1, 0)
        return remote(
            scores.at[slot], parts.at[rel, part], ps_send.at[slot], ps_recv.at[rel, part],
            {"dom": owner},
        )

    def evidence_of(peak, mass):
        return jnp.concatenate([peak, mass, peak, mass], axis=0)

    def stat_copies(h, src, slots, index, peers, ssem, rsem):
        out = [
            remote(src.at[h], slots.at[h, index], ssem.at[h, k], rsem.at[h, k], peers[k])
            for k in range(1, len(peers))
        ]
        back = [
            remote(
                src.at[h], slots.at[h, (index + len(peers) - k) % len(peers)],
                ssem.at[h, k], rsem.at[h, k], peers[k],
            )
            for k in range(1, len(peers))
        ]
        return out, back

    def merged(h, slots):
        both = slots[h]
        peak = jnp.max(both[:, :2], axis=0)
        return peak, jnp.sum(both[:, 2:4] * jnp.exp(both[:, :2] - peak[None]), axis=0)

    z_stats = lambda h: stat_copies(h, stat_a, stat_z, z0, z_peer, z_send, z_recv)
    q_stats = lambda h: stat_copies(h, stat_b, stat_q, q0, q_peer, q_send, q_recv)

    def sum_scores(h):
        peaks, masses = [], []
        for k in range(2):
            part = h * 2 + k
            mine = h * 2 * ND + dom * 2 + k
            total = scores[mine]
            for rel in range(ND - 1):
                remote(
                    scores.at[mine], parts.at[rel, part], ps_send.at[mine],
                    ps_recv.at[rel, part], d_peer[1],
                ).wait_recv()
                total = total + parts[rel, part]
            total = total * temp
            parts[0, part] = total
            peak = jnp.max(total, axis=0, keepdims=True)
            peaks.append(peak)
            masses.append(jnp.sum(jnp.exp(total - peak), axis=0, keepdims=True))
        tile = evidence_of(jnp.concatenate(peaks, axis=0), jnp.concatenate(masses, axis=0))
        stat_a[h] = tile
        stat_z[h, z0] = tile
        for c in z_stats(h)[0]:
            c.start()

    def merge_z(h):
        for c in z_stats(h)[1]:
            c.wait_recv()
        tile = evidence_of(*merged(h, stat_z))
        stat_b[h] = tile
        stat_q[h, q0] = tile
        for c in q_stats(h)[0]:
            c.start()

    weights = (weights_0, weights_1)

    def w_copy(h, n, owner, peer):
        ref = weights[h].at[:, pl.ds(pl.multiple_of(owner * share, share), share)]
        return remote(ref, ref, w_send.at[h, n], w_recv.at[h, n], peer)

    def l_copy(h, k, owner):
        ref = evid.at[h, owner]
        return remote(ref, ref, l_send.at[h, k], l_recv.at[h, k], d_peer[k])

    def weigh(h):
        for c in q_stats(h)[1]:
            c.wait_recv()
        peak, mass = merged(h, stat_q)
        log_evidence = peak + jnp.log(mass)
        for k in range(2):
            w = jnp.exp(parts[0, h * 2 + k] - log_evidence[k : k + 1])
            place = pl.ds(pl.multiple_of(dom * share + k * BATCH, BATCH), BATCH)
            weights[h][:, place] = w.astype(jnp.bfloat16)
        evid[h, dom] = evidence_of(log_evidence, mass)
        w_copy(h, 0, dom, side_peer).start()
        w_copy(h, 1, dom, chip_peer).start()
        for k in range(1, ND):
            l_copy(h, k, dom).start()

    def forward(h):
        w_copy(h, 0, side_dom, side_peer).wait_recv()
        w_copy(h, 2, side_dom, chip_peer).start()

    def receive(h):
        w_copy(h, 1, chip_dom, chip_peer).wait_recv()
        w_copy(h, 2, (chip_dom + 2) % ND, chip_peer).wait_recv()

    def first_numerator(piece):
        def step(j, carry):
            columns = pl.ds(pl.multiple_of(piece * quarter + j * 256, 256), 256)
            num[:, columns] = jnp.dot(
                weights_0[...], rows[:half, columns], preferred_element_type=jnp.float32
            )
            return carry

        lax.fori_loop(0, quarter // 256, step, 0)

    chain = (sum_scores, merge_z, weigh, forward, receive)

    ready = []

    def prepare():
        load.wait()
        lax.fori_loop(0, refs // 16, relayout, 0)
        total = jnp.zeros((refs, LANES), jnp.float32)
        for c in range(width // LANES):
            piece = temps[:, c * LANES : (c + 1) * LANES].astype(jnp.float32)
            total = total + piece * piece
        total = 0.5 * total
        for c in range(3):
            head = total.astype(jnp.bfloat16)
            power[c] = head
            total = total - head.astype(jnp.float32)
        edge[...] = temps[:, :LANES]
        lane = lax.broadcasted_iota(jnp.int32, (refs, LANES), 1)
        stash = (lane == LOW_AT) | (lane == HIGH_AT)
        temps[:, :LANES] = jnp.where(
            stash, jnp.zeros((refs, LANES), jnp.bfloat16), temps[:, :LANES]
        )

    def phase_body(phase, carry):
        for n, (issue, wanted) in enumerate(segments):

            @pl.when(phase == n)
            def _(n=n, issue=issue, wanted=wanted):
                for s in issue:
                    if isinstance(s, int):
                        chain[s](0)
                    else:
                        if s["needs"] is not None and n == 0 and not ready:
                            prepare()
                            ready.append(True)
                        hear(s["needs"])
                        copy_of(s, s["unit"]).start()
                for w in wanted:
                    hear(w)

        bh = table([b[0] for b in batches], phase)
        bz = (z0 + table([b[1] for b in batches], phase)) % NZ
        place = bz % ND * 2 + bz // ND
        slot = bh * 2 * ND + place
        here = pl.ds(pl.multiple_of(slot * BATCH, BATCH), BATCH)
        bounds = rows[here, :LANES].astype(jnp.float32)
        lane = lax.broadcasted_iota(jnp.int32, (BATCH, LANES), 1)
        bins = (lane * 37 % NBIN).astype(jnp.float32)
        seen = (bins >= bounds[:, LOW_AT : LOW_AT + 1]) & (bins < bounds[:, HIGH_AT : HIGH_AT + 1])
        mask = jnp.where(seen, 1.0, 0.0).astype(jnp.bfloat16)
        masks[here, :] = mask
        nt = (((1,), (1,)), ((), ()))
        penalty = lax.dot_general(power[2], mask, nt, preferred_element_type=jnp.float32)
        for c in (1, 0):
            penalty = penalty + lax.dot_general(
                power[c], mask, nt, preferred_element_type=jnp.float32
            )
        corr = lax.dot_general(temps[...], rows[here, :], nt, preferred_element_type=jnp.float32)
        scores[slot] = corr - penalty

        @pl.when(place // 2 != dom)
        def _():
            partial_copy(slot).start()

        return carry

    lax.fori_loop(0, len(segments), phase_body, 0)

    for step in late:
        chain[step](0)
    sum_scores(1)
    first_numerator(0)
    merge_z(1)
    first_numerator(1)
    for h in range(NH):
        sent = sum((s["hi"] - s["lo"]) * UNIT for s in sends if s["unit"][0] == h)
        assert sent * LANES % width == 0 and sent * LANES // width <= half
        every = rows.at[pl.ds(0, sent * LANES // width)]
        pltpu.make_async_copy(every, every, send_sem.at[h]).wait()
    weigh(1)

    def drain(slot, carry):
        @pl.when(slot % (2 * ND) // 2 != dom)
        def _():
            partial_copy(slot).wait_send()

        return carry

    lax.fori_loop(0, NH * 2 * ND, drain, 0)
    for k in range(1, ND):
        a_copy(k, dom, (dom + k) % ND).wait_send()
    den = jnp.dot(weights_0[...], masks[:half], preferred_element_type=jnp.float32)
    inverse[...] = den
    forward(1)
    for h in range(NH):
        for c in z_stats(h)[0] + q_stats(h)[0]:
            c.wait_send()
    receive(1)
    den = inverse[...] + jnp.dot(weights_1[...], masks[half:], preferred_element_type=jnp.float32)
    inverse[...] = 1.0 / (den + 1.0)
    for h in range(NH):
        for k in range(1, ND):
            l_copy(h, k, (dom + ND - k) % ND).wait_recv()
    for h in range(NH):
        for k in range(1, ND):
            l_copy(h, k, dom).wait_send()
        w_copy(h, 0, dom, side_peer).wait_send()
        w_copy(h, 1, dom, chip_peer).wait_send()
        w_copy(h, 2, side_dom, chip_peer).wait_send()


def update_kernel(weights, inverse, rows, num, temps, edge, evid, out, evid_out, staged, sems):
    refs, width = num.shape
    quarter, half = width // 2, weights.shape[1]
    tile = staged.shape[3]
    evid_out[...] = evid[...]

    def copy(j):
        columns = pl.ds(pl.multiple_of(j * tile, tile), tile)
        return pltpu.make_async_copy(staged.at[j % 2], out.at[:, :, columns], sems.at[j % 2])

    lane = lax.broadcasted_iota(jnp.int32, (refs, LANES), 1)
    stash = (lane == LOW_AT) | (lane == HIGH_AT)
    scale = jnp.concatenate([inverse[...]] * (tile // LANES), axis=1)

    def step(j, carry):
        @pl.when(j >= 2)
        def _():
            copy(j - 2).wait()

        for c in range(2):
            columns = pl.ds(pl.multiple_of(c * quarter + j * tile, tile), tile)
            total = num[:, columns] + jnp.dot(
                weights[...], rows[half:, columns], preferred_element_type=jnp.float32
            )
            staged[j % 2, :, c, :] = (total + temps[:, columns].astype(jnp.float32)) * scale

        @pl.when(j == 0)
        def _():
            first = staged[0, :, 0, :LANES]
            kept = edge[...].astype(jnp.float32) * inverse[...]
            staged[0, :, 0, :LANES] = jnp.where(stash, kept, first)

        copy(j).start()
        return carry

    steps = quarter // tile
    lax.fori_loop(0, steps, step, 0)
    copy(steps - 2).wait()
    copy(steps - 1).wait()


def on_device(particles, templates, tilt_low, tilt_high):
    local, _, band = particles.shape
    refs = templates.shape[0]
    quarter = band // ND
    width = 2 * quarter
    temp = 3.0 / math.sqrt(band)
    bounds = jnp.stack([tilt_low, tilt_high])

    schedule = plan(width // LANES, 13, 7, 10)
    line = timeline(schedule, (9.0, 6.0, 9.0, 8.0, 4.0))
    count = 1 + max(s["sem"] for s in schedule[0])
    total = NX * NY * NZ * ND * local
    half = total // NH
    bf16, f32 = jnp.bfloat16, jnp.float32
    dma = pltpu.SemaphoreType.DMA
    vmem = pl.BlockSpec(memory_space=pltpu.VMEM)
    rows, temps, edge, num, weights, inverse, evidence = pl.pallas_call(
        functools.partial(em_kernel, schedule[0], line, temp),
        out_shape=(
            jax.ShapeDtypeStruct((total, width), bf16),
            jax.ShapeDtypeStruct((refs, width), bf16),
            jax.ShapeDtypeStruct((refs, LANES), bf16),
            jax.ShapeDtypeStruct((refs, width), f32),
            jax.ShapeDtypeStruct((refs, half), bf16),
            jax.ShapeDtypeStruct((refs, LANES), f32),
            jax.ShapeDtypeStruct((NH, ND, 8, LANES), f32),
        ),
        in_specs=[
            pl.BlockSpec(memory_space=pltpu.HBM),
            pl.BlockSpec(memory_space=pltpu.SMEM),
            pl.BlockSpec(memory_space=pltpu.HBM),
        ],
        out_specs=(vmem,) * 7,
        scratch_shapes=[
            pltpu.VMEM(particles.shape, bf16),
            pltpu.VMEM((ND * local, width), bf16),
            pltpu.VMEM((refs, 2, quarter), bf16),
            pltpu.VMEM((total, LANES), bf16),
            pltpu.VMEM((refs, half), bf16),
            pltpu.VMEM((NH * 2 * ND, refs, LANES), f32),
            pltpu.VMEM((ND - 1, NH * 2, refs, LANES), f32),
            pltpu.VMEM((NH, 8, LANES), f32),
            pltpu.VMEM((NH, 8, LANES), f32),
            pltpu.VMEM((NH, NZ, 8, LANES), f32),
            pltpu.VMEM((NH, NX * NY, 8, LANES), f32),
            pltpu.VMEM((3, refs, LANES), bf16),
            dma(()),
            dma(()),
            dma((ND,)),
            dma((ND,)),
            dma((NH,)),
            dma((count,)),
            dma((NH * 2 * ND,)),
            dma((ND - 1, NH * 2)),
            dma((NH, NZ)),
            dma((NH, NZ)),
            dma((NH, NX * NY)),
            dma((NH, NX * NY)),
            dma((NH, 3)),
            dma((NH, 3)),
            dma((NH, ND)),
            dma((NH, ND)),
        ],
        compiler_params=pltpu.CompilerParams(
            collective_id=0, has_side_effects=True, vmem_limit_bytes=12 * 1024 * 1024
        ),
    )(
        pltpu.with_memory_space_constraint(particles, pltpu.HBM),
        bounds,
        pltpu.with_memory_space_constraint(templates, pltpu.HBM),
    )
    tile = 256
    updated, evidence = pl.pallas_call(
        update_kernel,
        out_shape=(
            jax.ShapeDtypeStruct((refs, 2, quarter), f32),
            jax.ShapeDtypeStruct(evidence.shape, f32),
        ),
        in_specs=[vmem] * 7,
        out_specs=(pl.BlockSpec(memory_space=pltpu.HBM), vmem),
        scratch_shapes=[pltpu.VMEM((2, refs, 2, tile), f32), dma((2,))],
        compiler_params=pltpu.CompilerParams(vmem_limit_bytes=8 * 1024 * 1024),
    )(weights, inverse, rows, num, temps, edge, evidence)
    evidence = evidence[:, :, :2].reshape(NH, ND, 2, NX, NY, 2, local)
    dom = lax.axis_index("dom")
    evidence = lax.dynamic_index_in_dim(evidence, dom // 2, 0, keepdims=False)
    evidence = lax.dynamic_index_in_dim(evidence, dom % 2, 4, keepdims=False)
    evidence = jnp.transpose(evidence, (2, 3, 1, 0, 4)).reshape(-1)
    return updated, evidence


def solution(mesh):
    in_specs = (
        P(("dom", "orient"), None, None),
        P("orient", None, None),
        P(("dom", "orient")),
        P(("dom", "orient")),
    )
    out_specs = (P("orient", None, "dom"), P("dom"))
    return jax.shard_map(
        on_device, mesh=mesh, in_specs=in_specs, out_specs=out_specs, check_vma=False
    )
```

```python
import functools
import math

import jax
import jax.numpy as jnp
from jax import lax
from jax.experimental import pallas as pl
from jax.experimental.pallas import tpu as pltpu
from jax.sharding import PartitionSpec as P

NBIN = 64
NX, NY, NZ, ND, NH = 2, 4, 8, 4, 2
LANES = 128
RING = (0, 7, 1, 6, 2, 5, 3, 4)
LINKS = ("x", "y+", "y-", "z+", "z-")
LATENCY = 3.75
TILE = 0.0879
AHEAD = 2.0
CUTS = ((13, 8, 14), (13, 8, 9))
RANKS = (3, 2, 2, 3, 0)
LAGS = (2.5, 11.0, 9.0)
PREPARE_AT, PREPARE_STEP, PREPARE_PARTS = 6.0, 3.0, 8
BATCH = 128
UNIT = 16
LOW_AT, HIGH_AT = 19, 83
MESH = pl.DeviceIdType.MESH


def moved(unit, link):
    h, x, z, y = unit
    if link == "x":
        return h, 1 - x, z, y
    step = -1 if link[1] == "+" else 1
    return (h, x, (z + step) % NZ, y) if link[0] == "z" else (h, x, z, (y + step) % NY)

def plan(cols, cuts, ranks=(0, 1, 2, 2, 3)):
    sends = []
    def add(link, unit, part, lo, hi, rank):
        sends.append(dict(link=link, unit=unit, part=part, lo=lo, hi=hi, rank=rank, lands=moved(unit, link)))
    for h in range(NH):
        first_a, second_a, x_cols = cuts[h]
        add("x", (h, 0, 0, 0), "F", 0, cols, 0)
        for x in (0, 1):
            cut, end = (first_a, cols) if x == 0 else (second_a, cols - x_cols)
            plus = (x + h) % 2 == 0
            add("y+", (h, x, 0, 0), "A", 0, cut, ranks[0])
            add("y-", (h, x, 0, 0), "A", 0, cut, ranks[0])
            link, y = ("y+", 3) if plus else ("y-", 1)
            add(link, (h, x, 0, y), "A", 0, cut, ranks[0])
            for k in range(4):
                if k < 3 or plus:
                    add("z+", (h, x, -k % NZ, 0), "B", cut, end, ranks[1])
                if k < 3 or not plus:
                    add("z-", (h, x, k, 0), "B", cut, end, ranks[1])
            for k in range(4):
                for y in (0, 3, 1, 2):
                    if k < 3 or y in (0, 3):
                        add("z+", (h, x, -k % NZ, y), "A", 0, cut, ranks[2])
                    if k < 3 or y in (1, 2):
                        add("z-", (h, x, k, y), "A", 0, cut, ranks[2])
            for n, z in enumerate(RING):
                add("y+", (h, x, z, 0), "B", cut, end, ranks[3])
                add("y-", (h, x, z, 0), "B", cut, end, ranks[3])
                link, y = ("y+", 3) if n % 2 == 0 else ("y-", 1)
                add(link, (h, x, z, y), "B", cut, end, ranks[3])
            if x == 0 and x_cols:
                for z in RING:
                    for y in (0, 3, 1, 2):
                        if (z, y) != (0, 0):
                            add("x", (h, 0, z, y), "X", cols - x_cols, cols, ranks[4])
    for number, s in enumerate(sends):
        s["id"] = number
    arrives = {(s["lands"], s["part"]): s["id"] for s in sends}
    for s in sends:
        h, x, z, y = s["unit"]
        if (x, z, y) == (0, 0, 0):
            s["needs"] = None
        elif (x, z, y) == (1, 0, 0):
            s["needs"] = arrives[s["unit"], "F"]
        else:
            s["needs"] = arrives[s["unit"], "B" if s["part"] == "X" else s["part"]]
    forwarded = {s["needs"] for s in sends}
    groups = {}
    for s in sends:
        key = (s["part"], s["lands"][:3]) if s["id"] not in forwarded else s["id"]
        groups.setdefault(key, []).append(s)
    for sem, members in enumerate(groups.values()):
        assert len({(s["lo"], s["hi"]) for s in members}) == 1
        for s in members:
            s["sem"], s["group"] = sem, len(members)
    free, landed, left = dict.fromkeys(LINKS, 0.0), {None: 0.0}, list(sends)
    when = {}; latest = dict.fromkeys(LINKS, 0.0)
    while left:
        best = None
        for s in left:
            if s["needs"] in landed:
                key = (max(landed[s["needs"]], free[s["link"]]), s["unit"][:2], s["rank"], s["id"])
                if best is None or key < best[0]:
                    best = key, s
        (start, *_), s = best
        free[s["link"]] = start + (s["hi"] - s["lo"]) * TILE
        landed[s["id"]] = free[s["link"]] + LATENCY
        early = start - AHEAD if s["part"] == "X" else 0.0
        latest[s["link"]] = max(latest[s["link"]], landed[s["needs"]], early)
        when[s["id"]] = latest[s["link"]]
        left.remove(s)
    events = [(when[s["id"]], 0, s["id"], s) for s in sends]
    batches = []
    for h in range(NH):
        for z in range(NZ):
            wanted = [arrives[(h, x, z, y), p] for x in range(NX) for y in range(NY) for p in "FABX" if ((h, x, z, y), p) in arrives]
            batches.append((max(landed[w] for w in wanted), h, z, wanted))
    batches.sort()
    return sends, events, batches, free


def timeline(schedule, lags):
    sends, events, batches, _ = schedule
    couples = [
        (two[1][0], two[0][1], (two[0][2], two[1][2]), two[0][3] + two[1][3])
        for two in zip(batches[::2], batches[1::2])
    ]
    assert all(one[1] == other[1] for one, other in zip(batches[::2], batches[1::2]))
    first = max(b[0] for b in couples if b[1] == 0)
    steps = [(first + sum(lags[: n + 1]), 2, n, None) for n in range(len(lags))]
    marked = [(b[0], 1, n, b) for n, b in enumerate(couples)]
    marked += [(PREPARE_AT + n * PREPARE_STEP, 3, n, None) for n in range(PREPARE_PARTS)]
    segments, issue, order = [], [], []
    for _, kind, n, what in sorted(events + marked + steps, key=lambda e: e[:3]):
        if kind == 1:
            segments.append((issue, what[3]))
            order.append((what[1], what[2]))
            issue = []
        else:
            issue.append(what if kind == 0 else (kind, n))
    assert not any(isinstance(e, dict) for e in issue)
    return segments, order, issue


def same(one, other):
    keys = ("link", "part", "lo", "hi")
    return all(one[k] == other[k] for k in keys)


def table(values, index):
    total = jnp.int32(0)
    for n, v in enumerate(values):
        if v:
            total = total + jnp.where(index == n, v, 0)
    return total


def em_kernel(
    sends, line, temp, whole_particles, bounds, templates,
    rows, temps, edge, num, weights_1, inverse, evid,
    particles, split, pairs, masks, weights_0, scores, core_parts, parts, totals, stat_a, stat_b, stat_z, stat_q, power,
    local_sem, load_sem, a_send, a_recv, send_sem, recv_sem,
    ps_send, pc_recv, px_recv, z_send, z_recv, q_send, q_recv, t_send, t_recv, l_send, l_recv,
):
    segments, batches, late = line
    dom, orient = lax.axis_index("dom"), lax.axis_index("orient")
    x0, y0, z0 = orient // (NY * NZ), (orient // NZ) % NY, orient % NZ
    q0 = x0 * NY + y0
    refs, width = temps.shape
    quarter = width // 2
    half = rows.shape[0] // NH
    share = half // ND

    def at(x, y, z):
        return {"orient": (x * NY + y) * NZ + z}

    z_peer = [at(x0, y0, (z0 + k) % NZ) for k in range(NZ)]
    q_peer = [{"orient": (q0 + k) % (NX * NY) * NZ + z0} for k in range(NX * NY)]
    d_peer = [{"dom": (dom + k) % ND} for k in range(ND)]
    target = {
        "x": q_peer[NY],
        "y+": at(x0, (y0 + 1) % NY, z0),
        "y-": at(x0, (y0 + NY - 1) % NY, z0),
        "z+": z_peer[1],
        "z-": z_peer[NZ - 1],
    }
    chip_dom = dom + 1 - 2 * (dom % 2)
    side_dom = (dom + 2) % ND
    chip_peer, side_peer = {"dom": chip_dom}, {"dom": side_dom}

    load = pltpu.make_async_copy(
        templates.at[:, :, pl.ds(pl.multiple_of(dom * quarter, quarter), quarter)],
        pairs,
        load_sem,
    )
    fetch = pltpu.make_async_copy(whole_particles, particles, local_sem)
    fetch.start()
    load.start()
    barrier = pltpu.get_barrier_semaphore()
    greeted = list(target.values()) + d_peer[1:]
    for peer in greeted:
        pl.semaphore_signal(barrier, inc=1, device_id=peer, device_id_type=MESH)

    def remote(src, dst, ssem, rsem, peer):
        return pltpu.make_async_remote_copy(
            src_ref=src, dst_ref=dst, send_sem=ssem, recv_sem=rsem,
            device_id=peer, device_id_type=MESH,
        )

    z_at = [
        ((z0 + k) % NZ % ND * 2 + (z0 + k) % NZ // ND) * BATCH for k in range(NZ)
    ]
    y_at = [(y0 + k) % NY * UNIT for k in range(NY)]
    x_at = [x0 * NY * UNIT, (1 - x0) * NY * UNIT]

    def unit_row(unit):
        h, x, z, y = unit
        return h * half + x_at[x] + z_at[z] + y_at[y]

    def relayout(i, carry):
        r = pl.ds(pl.multiple_of(i * 16, 16), 16)
        for c in range(2):
            temps[r, c * quarter : (c + 1) * quarter] = pairs[r, c, :]
        return carry

    local = particles.shape[0]
    item = lax.broadcasted_iota(jnp.int32, (local, 1), 0)
    low, high = jnp.zeros((local, 1), jnp.float32), jnp.zeros((local, 1), jnp.float32)
    for n in range(local):
        low = jnp.where(item == n, bounds[0, n].astype(jnp.float32), low)
        high = jnp.where(item == n, bounds[1, n].astype(jnp.float32), high)
    column = lax.broadcasted_iota(jnp.int32, (local, quarter), 1)
    bins = (column * 37 % NBIN).astype(jnp.float32)
    seen = (low <= bins) & (bins < high)
    stash = jnp.where(column == LOW_AT, low, jnp.where(column == HIGH_AT, high, 0.0))
    fetch.wait()
    for c in range(2):
        for d in range(ND):
            piece = particles[:, c, d * quarter : (d + 1) * quarter].astype(jnp.float32)
            piece = jnp.where(seen, piece, stash if c == 0 else 0.0)
            split[d * local : (d + 1) * local, c * quarter : (c + 1) * quarter] = piece.astype(
                jnp.bfloat16
            )
    pl.semaphore_wait(barrier, len(greeted))

    own_at = unit_row((0, 0, 0, 0))

    def split_at(owner):
        return split.at[pl.ds(pl.multiple_of(owner * local, local), local)]

    def own_rows(source):
        row = own_at + source // 2 * half + source % 2 * local
        return rows.at[pl.ds(pl.multiple_of(row, local), local)]

    diag_dom = (chip_dom + 2) % ND
    others = ((chip_dom, chip_peer), (side_dom, side_peer), (diag_dom, {"dom": diag_dom}))

    def a_copy(k, source, owner):
        return remote(split_at(owner), own_rows(source), a_send.at[k], a_recv.at[k], others[k][1])

    for k in (1, 2, 0):
        a_copy(k, dom, others[k][0]).start()
    own = pltpu.make_async_copy(split_at(dom), own_rows(dom), local_sem)
    own.start()

    def copy_of(s, unit):
        columns = pl.ds(s["lo"] * LANES, (s["hi"] - s["lo"]) * LANES)
        place = rows.at[pl.ds(pl.multiple_of(unit_row(unit), UNIT), UNIT), columns]
        return remote(
            place, place, send_sem.at[unit[0]], recv_sem.at[s["sem"]], target[s["link"]]
        )

    heard = set()

    def hear(number):
        if number is None or sends[number]["sem"] in heard:
            return
        s = sends[number]
        heard.add(s["sem"])
        h, x, z, _ = s["lands"]
        columns = pl.ds(s["lo"] * LANES, (s["hi"] - s["lo"]) * LANES)
        if s["group"] == 1:
            row = unit_row(s["lands"])
        else:
            row = h * half + x_at[x] + z_at[z]
        place = rows.at[pl.ds(pl.multiple_of(row, UNIT), UNIT * s["group"]), columns]
        remote(
            place, place, send_sem.at[h], recv_sem.at[s["sem"]], target[s["link"]]
        ).wait_recv()

    def owner_of(slot):
        return slot % (2 * ND) // 2

    def core_copy(slot):
        return remote(
            scores.at[slot], core_parts.at[slot], ps_send.at[slot], pc_recv.at[slot], chip_peer
        )

    def side_copy(slot):
        part = slot // (2 * ND) * 2 + slot % 2
        return remote(
            scores.at[slot], parts.at[part], ps_send.at[slot], px_recv.at[part], side_peer
        )

    def combine(slot):
        @pl.when(owner_of(slot) % 2 == dom % 2)
        def _():
            core_copy(slot).wait_recv()
            scores[slot] = scores[slot] + core_parts[slot]

            @pl.when(owner_of(slot) != dom)
            def _():
                side_copy(slot).start()

    def evidence_of(peak, mass):
        return jnp.concatenate([peak, mass, peak, mass], axis=0)

    def stat_copies(h, src, slots, index, peers, ssem, rsem):
        out = [
            remote(src.at[h], slots.at[h, index], ssem.at[h, k], rsem.at[h, k], peers[k])
            for k in range(1, len(peers))
        ]
        back = [
            remote(
                src.at[h], slots.at[h, (index + len(peers) - k) % len(peers)],
                ssem.at[h, k], rsem.at[h, k], peers[k],
            )
            for k in range(1, len(peers))
        ]
        return out, back

    def merged(h, slots):
        both = slots[h]
        peak = jnp.max(both[:, :2], axis=0)
        return peak, jnp.sum(both[:, 2:4] * jnp.exp(both[:, :2] - peak[None]), axis=0)

    z_stats = lambda h: stat_copies(h, stat_a, stat_z, z0, z_peer, z_send, z_recv)
    q_stats = lambda h: stat_copies(h, stat_b, stat_q, q0, q_peer, q_send, q_recv)

    def total_copy(h, n, k, owner, peer):
        ref = totals.at[h, owner, k]
        return remote(ref, ref, t_send.at[h, n, k], t_recv.at[h, n, k], peer)

    def sum_scores(h):
        peaks, masses = [], []
        for k in range(2):
            mine = h * 2 * ND + dom * 2 + k
            side_copy(mine).wait_recv()
            total = (scores[mine] + parts[h * 2 + k]) * temp
            totals[h, dom, k] = total
            peak = jnp.max(total, axis=0, keepdims=True)
            peaks.append(peak)
            masses.append(jnp.sum(jnp.exp(total - peak), axis=0, keepdims=True))
        tile = evidence_of(jnp.concatenate(peaks, axis=0), jnp.concatenate(masses, axis=0))
        stat_a[h] = tile
        stat_z[h, z0] = tile
        for c in z_stats(h)[0]:
            c.start()
        total_copy(h, 0, 0, dom, side_peer).start()
        for k in range(2):
            total_copy(h, 1, k, dom, chip_peer).start()

    def merge_z(h):
        for c in z_stats(h)[1]:
            c.wait_recv()
        tile = evidence_of(*merged(h, stat_z))
        stat_b[h] = tile
        stat_q[h, q0] = tile
        for c in q_stats(h)[0]:
            c.start()
        total_copy(h, 0, 1, dom, side_peer).start()

    weights = (weights_0, weights_1)

    def l_copy(h, k, owner):
        ref = evid.at[h, owner]
        return remote(ref, ref, l_send.at[h, k], l_recv.at[h, k], d_peer[k])

    def weigh(h):
        for c in q_stats(h)[1]:
            c.wait_recv()
        peak, mass = merged(h, stat_q)
        log_evidence = peak + jnp.log(mass)
        evid[h, dom] = evidence_of(log_evidence, mass)
        for k in range(1, ND):
            l_copy(h, k, dom).start()
        fill_weights(h, dom, log_evidence)

    def fill_weights(h, owner, log_evidence):
        for k in range(2):
            w = jnp.exp(totals[h, owner, k] - log_evidence[k : k + 1])
            place = pl.ds(pl.multiple_of(owner * share + k * BATCH, BATCH), BATCH)
            weights[h][:, place] = w.astype(jnp.bfloat16)

    def forward(h):
        for k in range(2):
            total_copy(h, 0, k, side_dom, side_peer).wait_recv()
            total_copy(h, 2, k, side_dom, chip_peer).start()

    def receive(h):
        for k in range(2):
            total_copy(h, 1, k, chip_dom, chip_peer).wait_recv()
            total_copy(h, 2, k, diag_dom, chip_peer).wait_recv()

    def fill_others(h):
        for k in range(1, ND):
            owner = (dom + ND - k) % ND
            l_copy(h, k, owner).wait_recv()
            fill_weights(h, owner, evid[h, owner][:2])

    def first_numerator(piece):
        columns = pl.ds(piece * quarter, quarter)
        num[:, columns] = jnp.dot(
            weights_0[...], rows[:half, columns], preferred_element_type=jnp.float32
        )

    last_of = [max(n for n, b in enumerate(batches) if b[0] == h) for h in range(NH)]
    assert last_of == [len(batches) // 2 - 1, len(batches) - 1]

    def combine_last(h):
        for slot in slots_of(last_of[h]):
            combine(slot)

    chain = (combine_last, sum_scores, merge_z)

    def prepare(part):
        if part == 0:
            load.wait()
        share_of = refs // 16 // PREPARE_PARTS
        lax.fori_loop(part * share_of, (part + 1) * share_of, relayout, 0)
        if part < PREPARE_PARTS - 1:
            return
        total = jnp.zeros((refs, LANES), jnp.float32)
        for c in range(width // LANES):
            piece = temps[:, c * LANES : (c + 1) * LANES].astype(jnp.float32)
            total = total + piece * piece
        total = 0.5 * total
        for c in range(3):
            head = total.astype(jnp.bfloat16)
            power[c] = head
            total = total - head.astype(jnp.float32)
        edge[...] = temps[:, :LANES]
        lane = lax.broadcasted_iota(jnp.int32, (refs, LANES), 1)
        stash = (lane == LOW_AT) | (lane == HIGH_AT)
        temps[:, :LANES] = jnp.where(
            stash, jnp.zeros((refs, LANES), jnp.bfloat16), temps[:, :LANES]
        )

    def slots_of(phase):
        bh = table([b[0] for b in batches], phase)
        slots = []
        for n in range(2):
            bz = (z0 + table([b[1][n] for b in batches], phase)) % NZ
            slots.append(bh * 2 * ND + bz % ND * 2 + bz // ND)
        return slots

    opening = [s for s in sends if s["needs"] is None]
    twins = [(s, next(t for t in opening if t["unit"][0] == 1 and same(s, t)))
             for s in opening if s["unit"][0] == 0]
    near = dom // 2
    own.wait()
    a_copy(0, chip_dom, dom).wait_recv()
    for h in (near, 1 - near):
        for s, t in twins:
            columns = pl.ds(s["lo"] * LANES, (s["hi"] - s["lo"]) * LANES)
            row = unit_row((h, 0, 0, 0))
            place = rows.at[pl.ds(pl.multiple_of(row, UNIT), UNIT), columns]
            sem = s["sem"] + h * (t["sem"] - s["sem"])
            remote(
                place, place, send_sem.at[h], recv_sem.at[sem], target[s["link"]]
            ).start()
        if h is near:
            for k in (1, 2):
                a_copy(k, others[k][0], dom).wait_recv()

    def phase_body(phase, carry):
        for n, (issue, wanted) in enumerate(segments):

            @pl.when(phase == n)
            def _(n=n, issue=issue, wanted=wanted):
                for s in issue:
                    if isinstance(s, dict) and s["needs"] is None:
                        continue
                    if isinstance(s, tuple):
                        if s[0] == 3:
                            prepare(s[1])
                        else:
                            chain[s[1]](0)
                    else:
                        hear(s["needs"])
                        copy_of(s, s["unit"]).start()
                for w in wanted:
                    hear(w)

        slots = slots_of(phase)
        heres = [pl.ds(pl.multiple_of(slot * BATCH, BATCH), BATCH) for slot in slots]
        lane = lax.broadcasted_iota(jnp.int32, (BATCH, LANES), 1)
        bins = (lane * 37 % NBIN).astype(jnp.float32)
        both = []
        for here in heres:
            lims = rows[here, :LANES].astype(jnp.float32)
            seen = (bins >= lims[:, LOW_AT : LOW_AT + 1]) & (bins < lims[:, HIGH_AT : HIGH_AT + 1])
            mask = jnp.where(seen, 1.0, 0.0).astype(jnp.bfloat16)
            masks[here, :] = mask
            both.append(mask)
        mask = jnp.concatenate(both, axis=0)
        nt = (((1,), (1,)), ((), ()))
        penalty = lax.dot_general(power[2], mask, nt, preferred_element_type=jnp.float32)
        for c in (1, 0):
            penalty = penalty + lax.dot_general(
                power[c], mask, nt, preferred_element_type=jnp.float32
            )
        batch = jnp.concatenate([rows[here, :] for here in heres], axis=0)
        corr = lax.dot_general(temps[...], batch, nt, preferred_element_type=jnp.float32)
        result = corr - penalty
        for n, slot in enumerate(slots):
            scores[slot] = result[:, n * BATCH : (n + 1) * BATCH]

            @pl.when(owner_of(slot) % 2 != dom % 2)
            def _(slot=slot):
                core_copy(slot).start()

        @pl.when((phase > 0) & (phase != last_of[0] + 1))
        def _():
            for slot in slots_of(phase - 1):
                combine(slot)

        return carry

    lax.fori_loop(0, len(segments), phase_body, 0)

    for step in late:
        chain[step[1]](0)
    combine_last(1)
    forward(0)
    sum_scores(1)
    weigh(0)
    receive(0)
    merge_z(1)
    fill_others(0)
    first_numerator(0)
    forward(1)
    for h in range(NH):
        sent = sum((s["hi"] - s["lo"]) * UNIT for s in sends if s["unit"][0] == h)
        assert sent * LANES % width == 0 and sent * LANES // width <= half
        every = rows.at[pl.ds(0, sent * LANES // width)]
        pltpu.make_async_copy(every, every, send_sem.at[h]).wait()
    first_numerator(1)
    receive(1)
    weigh(1)

    def drain(slot, carry):
        @pl.when(owner_of(slot) != dom)
        def _():
            core_copy(slot).wait_send()

        return carry

    lax.fori_loop(0, NH * 2 * ND, drain, 0)
    for k in range(ND - 1):
        a_copy(k, dom, others[k][0]).wait_send()
    for h in range(NH):
        for c in z_stats(h)[0] + q_stats(h)[0]:
            c.wait_send()
        for k in range(2):
            total_copy(h, 0, k, dom, side_peer).wait_send()
            total_copy(h, 1, k, dom, chip_peer).wait_send()
            total_copy(h, 2, k, side_dom, chip_peer).wait_send()
    den = jnp.dot(weights_0[...], masks[:half], preferred_element_type=jnp.float32)
    inverse[...] = den
    fill_others(1)
    den = inverse[...] + jnp.dot(weights_1[...], masks[half:], preferred_element_type=jnp.float32)
    inverse[...] = 1.0 / (den + 1.0)
    for h in range(NH):
        for k in range(1, ND):
            l_copy(h, k, dom).wait_send()


def update_kernel(weights, inverse, rows, num, temps, edge, evid, out, evid_out, staged, sems):
    refs, width = num.shape
    quarter, half = width // 2, weights.shape[1]
    tile = staged.shape[3]
    evid_out[...] = evid[...]

    def copy(j):
        columns = pl.ds(pl.multiple_of(j * tile, tile), tile)
        return pltpu.make_async_copy(staged.at[j % 2], out.at[:, :, columns], sems.at[j % 2])

    lane = lax.broadcasted_iota(jnp.int32, (refs, LANES), 1)
    stash = (lane == LOW_AT) | (lane == HIGH_AT)
    scale = jnp.concatenate([inverse[...]] * (tile // LANES), axis=1)

    def step(j, carry):
        @pl.when(j >= 2)
        def _():
            copy(j - 2).wait()

        for c in range(2):
            columns = pl.ds(pl.multiple_of(c * quarter + j * tile, tile), tile)
            total = num[:, columns] + jnp.dot(
                weights[...], rows[half:, columns], preferred_element_type=jnp.float32
            )
            staged[j % 2, :, c, :] = (total + temps[:, columns].astype(jnp.float32)) * scale

        @pl.when(j == 0)
        def _():
            first = staged[0, :, 0, :LANES]
            kept = edge[...].astype(jnp.float32) * inverse[...]
            staged[0, :, 0, :LANES] = jnp.where(stash, kept, first)

        copy(j).start()
        return carry

    steps = quarter // tile
    lax.fori_loop(0, steps, step, 0)
    copy(steps - 2).wait()
    copy(steps - 1).wait()


def on_device(particles, templates, tilt_low, tilt_high):
    local, _, band = particles.shape
    refs = templates.shape[0]
    quarter = band // ND
    width = 2 * quarter
    temp = 3.0 / math.sqrt(band)
    bounds = jnp.stack([tilt_low, tilt_high])

    schedule = plan(width // LANES, CUTS, RANKS)
    line = timeline(schedule, LAGS)
    count = 1 + max(s["sem"] for s in schedule[0])
    total = NX * NY * NZ * ND * local
    half = total // NH
    bf16, f32 = jnp.bfloat16, jnp.float32
    dma = pltpu.SemaphoreType.DMA
    vmem = pl.BlockSpec(memory_space=pltpu.VMEM)
    rows, temps, edge, num, weights, inverse, evidence = pl.pallas_call(
        functools.partial(em_kernel, schedule[0], line, temp),
        out_shape=(
            jax.ShapeDtypeStruct((total, width), bf16),
            jax.ShapeDtypeStruct((refs, width), bf16),
            jax.ShapeDtypeStruct((refs, LANES), bf16),
            jax.ShapeDtypeStruct((refs, width), f32),
            jax.ShapeDtypeStruct((refs, half), bf16),
            jax.ShapeDtypeStruct((refs, LANES), f32),
            jax.ShapeDtypeStruct((NH, ND, 8, LANES), f32),
        ),
        in_specs=[
            pl.BlockSpec(memory_space=pltpu.HBM),
            pl.BlockSpec(memory_space=pltpu.SMEM),
            pl.BlockSpec(memory_space=pltpu.HBM),
        ],
        out_specs=(vmem,) * 7,
        scratch_shapes=[
            pltpu.VMEM(particles.shape, bf16),
            pltpu.VMEM((ND * local, width), bf16),
            pltpu.VMEM((refs, 2, quarter), bf16),
            pltpu.VMEM((total, LANES), bf16),
            pltpu.VMEM((refs, half), bf16),
            pltpu.VMEM((NH * 2 * ND, refs, LANES), f32),
            pltpu.VMEM((NH * 2 * ND, refs, LANES), f32),
            pltpu.VMEM((NH * 2, refs, LANES), f32),
            pltpu.VMEM((NH, ND, 2, refs, LANES), f32),
            pltpu.VMEM((NH, 8, LANES), f32),
            pltpu.VMEM((NH, 8, LANES), f32),
            pltpu.VMEM((NH, NZ, 8, LANES), f32),
            pltpu.VMEM((NH, NX * NY, 8, LANES), f32),
            pltpu.VMEM((3, refs, LANES), bf16),
            dma(()),
            dma(()),
            dma((ND - 1,)),
            dma((ND - 1,)),
            dma((NH,)),
            dma((count,)),
            dma((NH * 2 * ND,)),
            dma((NH * 2 * ND,)),
            dma((NH * 2,)),
            dma((NH, NZ)),
            dma((NH, NZ)),
            dma((NH, NX * NY)),
            dma((NH, NX * NY)),
            dma((NH, 3, 2)),
            dma((NH, 3, 2)),
            dma((NH, ND)),
            dma((NH, ND)),
        ],
        compiler_params=pltpu.CompilerParams(
            collective_id=0, has_side_effects=True, vmem_limit_bytes=18 * 1024 * 1024
        ),
    )(
        pltpu.with_memory_space_constraint(particles, pltpu.HBM),
        bounds,
        pltpu.with_memory_space_constraint(templates, pltpu.HBM),
    )
    tile = 1024
    updated, evidence = pl.pallas_call(
        update_kernel,
        out_shape=(
            jax.ShapeDtypeStruct((refs, 2, quarter), f32),
            jax.ShapeDtypeStruct(evidence.shape, f32),
        ),
        in_specs=[vmem] * 7,
        out_specs=(pl.BlockSpec(memory_space=pltpu.HBM), vmem),
        scratch_shapes=[pltpu.VMEM((2, refs, 2, tile), f32), dma((2,))],
        compiler_params=pltpu.CompilerParams(vmem_limit_bytes=12 * 1024 * 1024),
    )(weights, inverse, rows, num, temps, edge, evidence)
    evidence = evidence[:, :, :2].reshape(NH, ND, 2, NX, NY, 2, local)
    dom = lax.axis_index("dom")
    evidence = lax.dynamic_index_in_dim(evidence, dom // 2, 0, keepdims=False)
    evidence = lax.dynamic_index_in_dim(evidence, dom % 2, 4, keepdims=False)
    evidence = jnp.transpose(evidence, (2, 3, 1, 0, 4)).reshape(-1)
    return updated, evidence


def solution(mesh):
    in_specs = (
        P(("dom", "orient"), None, None),
        P("orient", None, None),
        P(("dom", "orient")),
        P(("dom", "orient")),
    )
    out_specs = (P("orient", None, "dom"), P("dom"))
    return jax.shard_map(
        on_device, mesh=mesh, in_specs=in_specs, out_specs=out_specs, check_vma=False
    )
```

```python
import functools
import math

import jax
import jax.numpy as jnp
from jax import lax
from jax.experimental import pallas as pl
from jax.experimental.pallas import tpu as pltpu
from jax.sharding import PartitionSpec as P

NBIN = 64
NX, NY, NZ, ND, NH = 2, 4, 8, 4, 2
LANES = 128
RING = (0, 7, 1, 6, 2, 5, 3, 4)
LINKS = ("x", "y+", "y-", "z+", "z-")
LATENCY = 4.25
TILE = 0.0879
AHEAD = 2.0
CUTS = ((13, 9, 11), (13, 8, 10))
RANKS = (3, 0, 2, 3, 0)
LAGS = (2.5, 11.0, 9.0)
PREPARE_AT, PREPARE_STEP, PREPARE_PARTS = 6.0, 3.0, 8
BATCH = 128
UNIT = 16
LOW_AT, HIGH_AT = 19, 83
MESH = pl.DeviceIdType.MESH


def moved(unit, link):
    h, x, z, y = unit
    if link == "x":
        return h, 1 - x, z, y
    step = -1 if link[1] == "+" else 1
    return (h, x, (z + step) % NZ, y) if link[0] == "z" else (h, x, z, (y + step) % NY)

def plan(cols, cuts, ranks=(0, 1, 2, 2, 3)):
    sends = []
    def add(link, unit, part, lo, hi, rank):
        sends.append(dict(link=link, unit=unit, part=part, lo=lo, hi=hi, rank=rank, lands=moved(unit, link)))
    for h in range(NH):
        first_a, second_a, x_cols = cuts[h]
        add("x", (h, 0, 0, 0), "F", 0, cols, 0)
        for x in (0, 1):
            cut, end = (first_a, cols) if x == 0 else (second_a, cols - x_cols)
            plus = (x + h) % 2 == 0
            add("y+", (h, x, 0, 0), "A", 0, cut, ranks[0])
            add("y-", (h, x, 0, 0), "A", 0, cut, ranks[0])
            link, y = ("y+", 3) if plus else ("y-", 1)
            add(link, (h, x, 0, y), "A", 0, cut, ranks[0])
            for k in range(4):
                if k < 3 or plus:
                    add("z+", (h, x, -k % NZ, 0), "B", cut, end, ranks[1])
                if k < 3 or not plus:
                    add("z-", (h, x, k, 0), "B", cut, end, ranks[1])
            for k in range(4):
                for y in (0, 3, 1, 2):
                    if k < 3 or y in (0, 3):
                        add("z+", (h, x, -k % NZ, y), "A", 0, cut, ranks[2])
                    if k < 3 or y in (1, 2):
                        add("z-", (h, x, k, y), "A", 0, cut, ranks[2])
            for n, z in enumerate(RING):
                add("y+", (h, x, z, 0), "B", cut, end, ranks[3])
                add("y-", (h, x, z, 0), "B", cut, end, ranks[3])
                link, y = ("y+", 3) if n % 2 == 0 else ("y-", 1)
                add(link, (h, x, z, y), "B", cut, end, ranks[3])
            if x == 0 and x_cols:
                for z in RING:
                    for y in (0, 3, 1, 2):
                        if (z, y) != (0, 0):
                            add("x", (h, 0, z, y), "X", cols - x_cols, cols, ranks[4])
    for number, s in enumerate(sends):
        s["id"] = number
    arrives = {(s["lands"], s["part"]): s["id"] for s in sends}
    for s in sends:
        h, x, z, y = s["unit"]
        if (x, z, y) == (0, 0, 0):
            s["needs"] = None
        elif (x, z, y) == (1, 0, 0):
            s["needs"] = arrives[s["unit"], "F"]
        else:
            s["needs"] = arrives[s["unit"], "B" if s["part"] == "X" else s["part"]]
    forwarded = {s["needs"] for s in sends}
    groups = {}
    for s in sends:
        key = (s["part"], s["lands"][:3]) if s["id"] not in forwarded else s["id"]
        groups.setdefault(key, []).append(s)
    for sem, members in enumerate(groups.values()):
        assert len({(s["lo"], s["hi"]) for s in members}) == 1
        for s in members:
            s["sem"], s["group"] = sem, len(members)
    free, landed, left = dict.fromkeys(LINKS, 0.0), {None: 0.0}, list(sends)
    when = {}; latest = dict.fromkeys(LINKS, 0.0)
    while left:
        best = None
        for s in left:
            if s["needs"] in landed:
                key = (max(landed[s["needs"]], free[s["link"]]), s["unit"][:2], s["rank"], s["id"])
                if best is None or key < best[0]:
                    best = key, s
        (start, *_), s = best
        free[s["link"]] = start + (s["hi"] - s["lo"]) * TILE
        landed[s["id"]] = free[s["link"]] + LATENCY
        early = start - AHEAD if s["part"] == "X" else 0.0
        latest[s["link"]] = max(latest[s["link"]], landed[s["needs"]], early)
        when[s["id"]] = latest[s["link"]]
        left.remove(s)
    events = [(when[s["id"]], 0, s["id"], s) for s in sends]
    batches = []
    for h in range(NH):
        for z in range(NZ):
            wanted = [arrives[(h, x, z, y), p] for x in range(NX) for y in range(NY) for p in "FABX" if ((h, x, z, y), p) in arrives]
            batches.append((max(landed[w] for w in wanted), h, z, wanted))
    batches.sort()
    return sends, events, batches, free


def timeline(schedule, lags):
    sends, events, batches, _ = schedule
    couples = [
        (two[1][0], two[0][1], (two[0][2], two[1][2]), two[0][3] + two[1][3])
        for two in zip(batches[::2], batches[1::2])
    ]
    assert all(one[1] == other[1] for one, other in zip(batches[::2], batches[1::2]))
    first = max(b[0] for b in couples if b[1] == 0)
    steps = [(first + sum(lags[: n + 1]), 2, n, None) for n in range(len(lags))]
    marked = [(b[0], 1, n, b) for n, b in enumerate(couples)]
    marked += [(PREPARE_AT + n * PREPARE_STEP, 3, n, None) for n in range(PREPARE_PARTS)]
    segments, issue, order = [], [], []
    for _, kind, n, what in sorted(events + marked + steps, key=lambda e: e[:3]):
        if kind == 1:
            segments.append((issue, what[3]))
            order.append((what[1], what[2]))
            issue = []
        else:
            issue.append(what if kind == 0 else (kind, n))
    assert not any(isinstance(e, dict) for e in issue)
    return segments, order, issue


def same(one, other):
    keys = ("link", "part", "lo", "hi")
    return all(one[k] == other[k] for k in keys)


def table(values, index):
    total = jnp.int32(0)
    for n, v in enumerate(values):
        if v:
            total = total + jnp.where(index == n, v, 0)
    return total


def em_kernel(
    sends, line, temp, whole_particles, bounds, templates,
    rows, temps, edge, num, weights_1, inverse, evid,
    particles, split, pairs, masks, weights_0, scores, core_parts, parts, totals, stat_a, stat_b, stat_z, stat_q, stat_w, power,
    local_sem, load_sem, a_send, a_recv, send_sem, recv_sem,
    ps_send, pc_recv, px_recv, z_send, z_recv, q_send, q_recv, t_send, t_recv, l_send, l_recv,
):
    segments, batches, late = line
    dom, orient = lax.axis_index("dom"), lax.axis_index("orient")
    x0, y0, z0 = orient // (NY * NZ), (orient // NZ) % NY, orient % NZ
    q0 = x0 * NY + y0
    refs, width = temps.shape
    quarter = width // 2
    half = rows.shape[0] // NH
    share = half // ND

    def at(x, y, z):
        return {"orient": (x * NY + y) * NZ + z}

    z_peer = [at(x0, y0, (z0 + k) % NZ) for k in range(NZ)]
    q_peer = [{"orient": (q0 + k) % (NX * NY) * NZ + z0} for k in range(NX * NY)]
    d_peer = [{"dom": (dom + k) % ND} for k in range(ND)]
    target = {
        "x": q_peer[NY],
        "y+": at(x0, (y0 + 1) % NY, z0),
        "y-": at(x0, (y0 + NY - 1) % NY, z0),
        "z+": z_peer[1],
        "z-": z_peer[NZ - 1],
    }
    chip_dom = dom + 1 - 2 * (dom % 2)
    side_dom = (dom + 2) % ND
    chip_peer, side_peer = {"dom": chip_dom}, {"dom": side_dom}

    load = pltpu.make_async_copy(
        templates.at[:, :, pl.ds(pl.multiple_of(dom * quarter, quarter), quarter)],
        pairs,
        load_sem,
    )
    fetch = pltpu.make_async_copy(whole_particles, particles, local_sem)
    fetch.start()
    load.start()
    barrier = pltpu.get_barrier_semaphore()
    greeted = list(target.values()) + d_peer[1:]
    for peer in greeted:
        pl.semaphore_signal(barrier, inc=1, device_id=peer, device_id_type=MESH)

    def remote(src, dst, ssem, rsem, peer):
        return pltpu.make_async_remote_copy(
            src_ref=src, dst_ref=dst, send_sem=ssem, recv_sem=rsem,
            device_id=peer, device_id_type=MESH,
        )

    z_at = [
        ((z0 + k) % NZ % ND * 2 + (z0 + k) % NZ // ND) * BATCH for k in range(NZ)
    ]
    y_at = [(y0 + k) % NY * UNIT for k in range(NY)]
    x_at = [x0 * NY * UNIT, (1 - x0) * NY * UNIT]

    def unit_row(unit):
        h, x, z, y = unit
        return h * half + x_at[x] + z_at[z] + y_at[y]

    def relayout(i, carry):
        r = pl.ds(pl.multiple_of(i * 16, 16), 16)
        for c in range(2):
            temps[r, c * quarter : (c + 1) * quarter] = pairs[r, c, :]
        return carry

    local = particles.shape[0]
    item = lax.broadcasted_iota(jnp.int32, (local, 1), 0)
    low, high = jnp.zeros((local, 1), jnp.float32), jnp.zeros((local, 1), jnp.float32)
    for n in range(local):
        low = jnp.where(item == n, bounds[0, n].astype(jnp.float32), low)
        high = jnp.where(item == n, bounds[1, n].astype(jnp.float32), high)
    column = lax.broadcasted_iota(jnp.int32, (local, quarter), 1)
    bins = (column * 37 % NBIN).astype(jnp.float32)
    seen = (low <= bins) & (bins < high)
    stash = jnp.where(column == LOW_AT, low, jnp.where(column == HIGH_AT, high, 0.0))
    fetch.wait()
    for c in range(2):
        for d in range(ND):
            piece = particles[:, c, d * quarter : (d + 1) * quarter].astype(jnp.float32)
            piece = jnp.where(seen, piece, stash if c == 0 else 0.0)
            split[d * local : (d + 1) * local, c * quarter : (c + 1) * quarter] = piece.astype(
                jnp.bfloat16
            )
    pl.semaphore_wait(barrier, len(greeted))

    own_at = unit_row((0, 0, 0, 0))

    def split_at(owner):
        return split.at[pl.ds(pl.multiple_of(owner * local, local), local)]

    def own_rows(source):
        row = own_at + source // 2 * half + source % 2 * local
        return rows.at[pl.ds(pl.multiple_of(row, local), local)]

    diag_dom = (chip_dom + 2) % ND
    others = ((chip_dom, chip_peer), (side_dom, side_peer), (diag_dom, {"dom": diag_dom}))

    def a_copy(k, source, owner):
        return remote(split_at(owner), own_rows(source), a_send.at[k], a_recv.at[k], others[k][1])

    for k in (1, 2, 0):
        a_copy(k, dom, others[k][0]).start()
    own = pltpu.make_async_copy(split_at(dom), own_rows(dom), local_sem)
    own.start()

    def copy_of(s, unit):
        columns = pl.ds(s["lo"] * LANES, (s["hi"] - s["lo"]) * LANES)
        place = rows.at[pl.ds(pl.multiple_of(unit_row(unit), UNIT), UNIT), columns]
        return remote(
            place, place, send_sem.at[unit[0]], recv_sem.at[s["sem"]], target[s["link"]]
        )

    heard = set()

    def hear(number):
        if number is None or sends[number]["sem"] in heard:
            return
        s = sends[number]
        heard.add(s["sem"])
        h, x, z, _ = s["lands"]
        columns = pl.ds(s["lo"] * LANES, (s["hi"] - s["lo"]) * LANES)
        if s["group"] == 1:
            row = unit_row(s["lands"])
        else:
            row = h * half + x_at[x] + z_at[z]
        place = rows.at[pl.ds(pl.multiple_of(row, UNIT), UNIT * s["group"]), columns]
        remote(
            place, place, send_sem.at[h], recv_sem.at[s["sem"]], target[s["link"]]
        ).wait_recv()

    def owner_of(slot):
        return slot % (2 * ND) // 2

    def core_copy(slot):
        return remote(
            scores.at[slot], core_parts.at[slot], ps_send, pc_recv.at[slot], chip_peer
        )

    def side_copy(slot):
        part = slot // (2 * ND) * 2 + slot % 2
        return remote(
            scores.at[slot], parts.at[part], ps_send, px_recv.at[part], side_peer
        )

    def combine(slot):
        @pl.when(owner_of(slot) % 2 == dom % 2)
        def _():
            core_copy(slot).wait_recv()
            scores[slot] = scores[slot] + core_parts[slot]

            @pl.when(owner_of(slot) != dom)
            def _():
                side_copy(slot).start()

    def evidence_of(peak, mass):
        return jnp.concatenate([peak, mass, peak, mass], axis=0)

    def send_stats(src, slot, peers, ssem, rsem):
        for peer in peers:
            remote(src, slot, ssem, rsem, peer).start()

    def all_but_one(slots, sem):
        most = slots.at[pl.ds(0, slots.shape[0] - 1)]
        return pltpu.make_async_copy(most, most, sem)

    def merged(both):
        peak = jnp.max(both[:, :2], axis=0)
        return peak, jnp.sum(both[:, 2:4] * jnp.exp(both[:, :2] - peak[None]), axis=0)

    def total_copy(h, n, k, owner, peer):
        ref = totals.at[h, owner, k]
        return remote(ref, ref, t_send.at[h], t_recv.at[h, n, k], peer)

    def sum_scores(h):
        peaks, masses = [], []
        for k in range(2):
            mine = h * 2 * ND + dom * 2 + k
            side_copy(mine).wait_recv()
            total = (scores[mine] + parts[h * 2 + k]) * temp
            totals[h, dom, k] = total
            peak = jnp.max(total, axis=0, keepdims=True)
            peaks.append(peak)
            masses.append(jnp.sum(jnp.exp(total - peak), axis=0, keepdims=True))
        tile = evidence_of(jnp.concatenate(peaks, axis=0), jnp.concatenate(masses, axis=0))
        stat_a[h] = tile
        stat_z[h, z0] = tile
        send_stats(stat_a.at[h], stat_z.at[h, z0], z_peer[1:], z_send.at[h], z_recv.at[h])
        total_copy(h, 0, 0, dom, side_peer).start()
        for k in range(2):
            total_copy(h, 1, k, dom, chip_peer).start()

    def merge_z(h):
        all_but_one(stat_z.at[h], z_recv.at[h]).wait()
        tile = evidence_of(*merged(stat_z[h]))
        stat_b[h] = tile
        if h == 0:
            stat_q[q0] = tile
            send_stats(stat_b.at[0], stat_q.at[q0], q_peer[1:], q_send.at[0], q_recv.at[0])
        else:
            slot = dom * NX * NY + q0
            stat_w[slot] = tile
            wide = [
                dict(q_peer[n % (NX * NY)], **d_peer[n // (NX * NY)])
                for n in range(1, ND * NX * NY)
            ]
            send_stats(stat_b.at[1], stat_w.at[slot], wide, q_send.at[1], q_recv.at[1])
        total_copy(h, 0, 1, dom, side_peer).start()

    weights = (weights_0, weights_1)

    def l_copy(k, owner):
        ref = evid.at[0, owner]
        return remote(ref, ref, l_send.at[k], l_recv.at[k], d_peer[k])

    def weigh_first():
        all_but_one(stat_q, q_recv.at[0]).wait()
        peak, mass = merged(stat_q[...])
        log_evidence = peak + jnp.log(mass)
        evid[0, dom] = evidence_of(log_evidence, mass)
        for k in range(1, ND):
            l_copy(k, dom).start()
        fill_weights(0, dom, log_evidence)

    def weigh_second():
        all_but_one(stat_w, q_recv.at[1]).wait()
        for owner in range(ND):
            peak, mass = merged(stat_w[owner * NX * NY : (owner + 1) * NX * NY])
            log_evidence = peak + jnp.log(mass)
            evid[1, owner] = evidence_of(log_evidence, mass)
            fill_weights(1, owner, log_evidence)

    def fill_weights(h, owner, log_evidence):
        for k in range(2):
            w = jnp.exp(totals[h, owner, k] - log_evidence[k : k + 1])
            place = pl.ds(pl.multiple_of(owner * share + k * BATCH, BATCH), BATCH)
            weights[h][:, place] = w.astype(jnp.bfloat16)

    def forward(h):
        for k in range(2):
            total_copy(h, 0, k, side_dom, side_peer).wait_recv()
            total_copy(h, 2, k, side_dom, chip_peer).start()

    def receive(h):
        for k in range(2):
            total_copy(h, 1, k, chip_dom, chip_peer).wait_recv()
            total_copy(h, 2, k, diag_dom, chip_peer).wait_recv()

    def fill_others():
        for k in range(1, ND):
            owner = (dom + ND - k) % ND
            l_copy(k, owner).wait_recv()
            fill_weights(0, owner, evid[0, owner][:2])

    def first_numerator(piece):
        columns = pl.ds(piece * quarter, quarter)
        num[:, columns] = jnp.dot(
            weights_0[...], rows[:half, columns], preferred_element_type=jnp.float32
        )

    last_of = [max(n for n, b in enumerate(batches) if b[0] == h) for h in range(NH)]
    assert last_of == [len(batches) // 2 - 1, len(batches) - 1]

    def combine_last(h):
        for slot in slots_of(last_of[h]):
            combine(slot)

    chain = (combine_last, sum_scores, merge_z)

    def prepare(part):
        if part == 0:
            load.wait()
        share_of = refs // 16 // PREPARE_PARTS
        lax.fori_loop(part * share_of, (part + 1) * share_of, relayout, 0)
        if part < PREPARE_PARTS - 1:
            return
        total = jnp.zeros((refs, LANES), jnp.float32)
        for c in range(width // LANES):
            piece = temps[:, c * LANES : (c + 1) * LANES].astype(jnp.float32)
            total = total + piece * piece
        total = 0.5 * total
        for c in range(3):
            head = total.astype(jnp.bfloat16)
            power[c] = head
            total = total - head.astype(jnp.float32)
        edge[...] = temps[:, :LANES]
        lane = lax.broadcasted_iota(jnp.int32, (refs, LANES), 1)
        stash = (lane == LOW_AT) | (lane == HIGH_AT)
        temps[:, :LANES] = jnp.where(
            stash, jnp.zeros((refs, LANES), jnp.bfloat16), temps[:, :LANES]
        )

    def slots_of(phase):
        bh = table([b[0] for b in batches], phase)
        slots = []
        for n in range(2):
            bz = (z0 + table([b[1][n] for b in batches], phase)) % NZ
            slots.append(bh * 2 * ND + bz % ND * 2 + bz // ND)
        return slots

    opening = [s for s in sends if s["needs"] is None]
    twins = [(s, next(t for t in opening if t["unit"][0] == 1 and same(s, t)))
             for s in opening if s["unit"][0] == 0]
    near = dom // 2
    own.wait()
    a_copy(0, chip_dom, dom).wait_recv()
    for h in (near, 1 - near):
        for s, t in twins:
            columns = pl.ds(s["lo"] * LANES, (s["hi"] - s["lo"]) * LANES)
            row = unit_row((h, 0, 0, 0))
            place = rows.at[pl.ds(pl.multiple_of(row, UNIT), UNIT), columns]
            sem = s["sem"] + h * (t["sem"] - s["sem"])
            remote(
                place, place, send_sem.at[h], recv_sem.at[sem], target[s["link"]]
            ).start()
        if h is near:
            for k in (1, 2):
                a_copy(k, others[k][0], dom).wait_recv()

    def phase_body(phase, carry):
        for n, (issue, wanted) in enumerate(segments):

            @pl.when(phase == n)
            def _(n=n, issue=issue, wanted=wanted):
                for s in issue:
                    if isinstance(s, dict) and s["needs"] is None:
                        continue
                    if isinstance(s, tuple):
                        if s[0] == 3:
                            prepare(s[1])
                        else:
                            chain[s[1]](0)
                    else:
                        hear(s["needs"])
                        copy_of(s, s["unit"]).start()
                for w in wanted:
                    hear(w)

        slots = slots_of(phase)
        heres = [pl.ds(pl.multiple_of(slot * BATCH, BATCH), BATCH) for slot in slots]
        lane = lax.broadcasted_iota(jnp.int32, (BATCH, LANES), 1)
        bins = (lane * 37 % NBIN).astype(jnp.float32)
        both = []
        for here in heres:
            lims = rows[here, :LANES].astype(jnp.float32)
            seen = (bins >= lims[:, LOW_AT : LOW_AT + 1]) & (bins < lims[:, HIGH_AT : HIGH_AT + 1])
            mask = jnp.where(seen, 1.0, 0.0).astype(jnp.bfloat16)
            masks[here, :] = mask
            both.append(mask)
        mask = jnp.concatenate(both, axis=0)
        nt = (((1,), (1,)), ((), ()))
        penalty = lax.dot_general(power[2], mask, nt, preferred_element_type=jnp.float32)
        for c in (1, 0):
            penalty = penalty + lax.dot_general(
                power[c], mask, nt, preferred_element_type=jnp.float32
            )
        batch = jnp.concatenate([rows[here, :] for here in heres], axis=0)
        corr = lax.dot_general(temps[...], batch, nt, preferred_element_type=jnp.float32)
        result = corr - penalty
        for n, slot in enumerate(slots):
            scores[slot] = result[:, n * BATCH : (n + 1) * BATCH]

            @pl.when(owner_of(slot) % 2 != dom % 2)
            def _(slot=slot):
                core_copy(slot).start()

        @pl.when((phase > 0) & (phase != last_of[0] + 1))
        def _():
            for slot in slots_of(phase - 1):
                combine(slot)

        return carry

    lax.fori_loop(0, len(segments), phase_body, 0)

    for step in late:
        chain[step[1]](0)
    combine_last(1)
    forward(0)
    sum_scores(1)
    weigh_first()
    receive(0)
    merge_z(1)
    fill_others()
    first_numerator(0)
    forward(1)
    for h in range(NH):
        sent = sum((s["hi"] - s["lo"]) * UNIT for s in sends if s["unit"][0] == h)
        assert sent * LANES % width == 0 and sent * LANES // width <= half
        every = rows.at[pl.ds(0, sent * LANES // width)]
        pltpu.make_async_copy(every, every, send_sem.at[h]).wait()
    first_numerator(1)
    receive(1)
    den = jnp.dot(weights_0[...], masks[:half], preferred_element_type=jnp.float32)
    inverse[...] = den

    for k in range(ND - 1):
        a_copy(k, dom, others[k][0]).wait_send()
    sent = scores.at[pl.ds(0, (NH * 2 * ND) * 3 // 4)]
    pltpu.make_async_copy(sent, sent, ps_send).wait()
    for h in range(NH):
        all_but_one(stat_z.at[h], z_send.at[h]).wait()
        sent = totals.at[h, pl.ds(0, 3)]
        pltpu.make_async_copy(sent, sent, t_send.at[h]).wait()
    all_but_one(stat_q, q_send.at[0]).wait()
    for k in range(1, ND):
        l_copy(k, dom).wait_send()
    weigh_second()
    den = inverse[...] + jnp.dot(weights_1[...], masks[half:], preferred_element_type=jnp.float32)
    inverse[...] = 1.0 / (den + 1.0)
    all_but_one(stat_w, q_send.at[1]).wait()


def update_kernel(weights, inverse, rows, num, temps, edge, evid, out, evid_out, staged, sems):
    refs, width = num.shape
    quarter, half = width // 2, weights.shape[1]
    tile = staged.shape[3]
    evid_out[...] = evid[...]

    def copy(j):
        columns = pl.ds(pl.multiple_of(j * tile, tile), tile)
        return pltpu.make_async_copy(staged.at[j % 2], out.at[:, :, columns], sems.at[j % 2])

    lane = lax.broadcasted_iota(jnp.int32, (refs, LANES), 1)
    stash = (lane == LOW_AT) | (lane == HIGH_AT)
    scale = jnp.concatenate([inverse[...]] * (tile // LANES), axis=1)

    def step(j, carry):
        @pl.when(j >= 2)
        def _():
            copy(j - 2).wait()

        for c in range(2):
            columns = pl.ds(pl.multiple_of(c * quarter + j * tile, tile), tile)
            total = num[:, columns] + jnp.dot(
                weights[...], rows[half:, columns], preferred_element_type=jnp.float32
            )
            staged[j % 2, :, c, :] = (total + temps[:, columns].astype(jnp.float32)) * scale

        @pl.when(j == 0)
        def _():
            first = staged[0, :, 0, :LANES]
            kept = edge[...].astype(jnp.float32) * inverse[...]
            staged[0, :, 0, :LANES] = jnp.where(stash, kept, first)

        copy(j).start()
        return carry

    steps = quarter // tile
    lax.fori_loop(0, steps, step, 0)
    copy(steps - 2).wait()
    copy(steps - 1).wait()


def on_device(particles, templates, tilt_low, tilt_high):
    local, _, band = particles.shape
    refs = templates.shape[0]
    quarter = band // ND
    width = 2 * quarter
    temp = 3.0 / math.sqrt(band)
    bounds = jnp.stack([tilt_low, tilt_high])

    schedule = plan(width // LANES, CUTS, RANKS)
    line = timeline(schedule, LAGS)
    count = 1 + max(s["sem"] for s in schedule[0])
    total = NX * NY * NZ * ND * local
    half = total // NH
    bf16, f32 = jnp.bfloat16, jnp.float32
    dma = pltpu.SemaphoreType.DMA
    vmem = pl.BlockSpec(memory_space=pltpu.VMEM)
    rows, temps, edge, num, weights, inverse, evidence = pl.pallas_call(
        functools.partial(em_kernel, schedule[0], line, temp),
        out_shape=(
            jax.ShapeDtypeStruct((total, width), bf16),
            jax.ShapeDtypeStruct((refs, width), bf16),
            jax.ShapeDtypeStruct((refs, LANES), bf16),
            jax.ShapeDtypeStruct((refs, width), f32),
            jax.ShapeDtypeStruct((refs, half), bf16),
            jax.ShapeDtypeStruct((refs, LANES), f32),
            jax.ShapeDtypeStruct((NH, ND, 8, LANES), f32),
        ),
        in_specs=[
            pl.BlockSpec(memory_space=pltpu.HBM),
            pl.BlockSpec(memory_space=pltpu.SMEM),
            pl.BlockSpec(memory_space=pltpu.HBM),
        ],
        out_specs=(vmem,) * 7,
        scratch_shapes=[
            pltpu.VMEM(particles.shape, bf16),
            pltpu.VMEM((ND * local, width), bf16),
            pltpu.VMEM((refs, 2, quarter), bf16),
            pltpu.VMEM((total, LANES), bf16),
            pltpu.VMEM((refs, half), bf16),
            pltpu.VMEM((NH * 2 * ND, refs, LANES), f32),
            pltpu.VMEM((NH * 2 * ND, refs, LANES), f32),
            pltpu.VMEM((NH * 2, refs, LANES), f32),
            pltpu.VMEM((NH, ND, 2, refs, LANES), f32),
            pltpu.VMEM((NH, 8, LANES), f32),
            pltpu.VMEM((NH, 8, LANES), f32),
            pltpu.VMEM((NH, NZ, 8, LANES), f32),
            pltpu.VMEM((NX * NY, 8, LANES), f32),
            pltpu.VMEM((ND * NX * NY, 8, LANES), f32),
            pltpu.VMEM((3, refs, LANES), bf16),
            dma(()),
            dma(()),
            dma((ND - 1,)),
            dma((ND - 1,)),
            dma((NH,)),
            dma((count,)),
            dma(()),
            dma((NH * 2 * ND,)),
            dma((NH * 2,)),
            dma((NH,)),
            dma((NH,)),
            dma((NH,)),
            dma((NH,)),
            dma((NH,)),
            dma((NH, 3, 2)),
            dma((ND,)),
            dma((ND,)),
        ],
        compiler_params=pltpu.CompilerParams(
            collective_id=0, has_side_effects=True, vmem_limit_bytes=18 * 1024 * 1024
        ),
    )(
        pltpu.with_memory_space_constraint(particles, pltpu.HBM),
        bounds,
        pltpu.with_memory_space_constraint(templates, pltpu.HBM),
    )
    tile = 1024
    updated, evidence = pl.pallas_call(
        update_kernel,
        out_shape=(
            jax.ShapeDtypeStruct((refs, 2, quarter), f32),
            jax.ShapeDtypeStruct(evidence.shape, f32),
        ),
        in_specs=[vmem] * 7,
        out_specs=(pl.BlockSpec(memory_space=pltpu.HBM), vmem),
        scratch_shapes=[pltpu.VMEM((2, refs, 2, tile), f32), dma((2,))],
        compiler_params=pltpu.CompilerParams(vmem_limit_bytes=12 * 1024 * 1024),
    )(weights, inverse, rows, num, temps, edge, evidence)
    evidence = evidence[:, :, :2].reshape(NH, ND, 2, NX, NY, 2, local)
    dom = lax.axis_index("dom")
    evidence = lax.dynamic_index_in_dim(evidence, dom // 2, 0, keepdims=False)
    evidence = lax.dynamic_index_in_dim(evidence, dom % 2, 4, keepdims=False)
    evidence = jnp.transpose(evidence, (2, 3, 1, 0, 4)).reshape(-1)
    return updated, evidence


def solution(mesh):
    in_specs = (
        P(("dom", "orient"), None, None),
        P("orient", None, None),
        P(("dom", "orient")),
        P(("dom", "orient")),
    )
    out_specs = (P("orient", None, "dom"), P("dom"))
    return jax.shard_map(
        on_device, mesh=mesh, in_specs=in_specs, out_specs=out_specs, check_vma=False
    )
```

```python
import functools
import math

import jax
import jax.numpy as jnp
from jax import lax
from jax.experimental import pallas as pl
from jax.experimental.pallas import tpu as pltpu
from jax.sharding import PartitionSpec as P

NBIN = 64
NX, NY, NZ, ND, NH = 2, 4, 8, 4, 2
LANES = 128
RING = (0, 7, 1, 6, 2, 5, 3, 4)
LINKS = ("x", "y+", "y-", "z+", "z-")
LATENCY = 4.25
TILE = 0.0879
AHEAD = 2.0
CUTS = ((13, 9, 11), (13, 8, 10))
RANKS = (3, 0, 2, 3, 0)
LAGS = (2.5, 11.0, 9.0)
PREPARE_AT, PREPARE_STEP, PREPARE_PARTS = 6.0, 3.0, 8
BATCH = 128
UNIT = 16
LOW_AT, HIGH_AT = 19, 83
MESH = pl.DeviceIdType.MESH


def moved(unit, link):
    h, x, z, y = unit
    if link == "x":
        return h, 1 - x, z, y
    step = -1 if link[1] == "+" else 1
    return (h, x, (z + step) % NZ, y) if link[0] == "z" else (h, x, z, (y + step) % NY)

def plan(cols, cuts, ranks=(0, 1, 2, 2, 3)):
    sends = []
    def add(link, unit, part, lo, hi, rank):
        sends.append(dict(link=link, unit=unit, part=part, lo=lo, hi=hi, rank=rank, lands=moved(unit, link)))
    for h in range(NH):
        first_a, second_a, x_cols = cuts[h]
        add("x", (h, 0, 0, 0), "F", 0, cols, 0)
        for x in (0, 1):
            cut, end = (first_a, cols) if x == 0 else (second_a, cols - x_cols)
            plus = (x + h) % 2 == 0
            add("y+", (h, x, 0, 0), "A", 0, cut, ranks[0])
            add("y-", (h, x, 0, 0), "A", 0, cut, ranks[0])
            link, y = ("y+", 3) if plus else ("y-", 1)
            add(link, (h, x, 0, y), "A", 0, cut, ranks[0])
            for k in range(4):
                if k < 3 or plus:
                    add("z+", (h, x, -k % NZ, 0), "B", cut, end, ranks[1])
                if k < 3 or not plus:
                    add("z-", (h, x, k, 0), "B", cut, end, ranks[1])
            for k in range(4):
                for y in (0, 3, 1, 2):
                    if k < 3 or y in (0, 3):
                        add("z+", (h, x, -k % NZ, y), "A", 0, cut, ranks[2])
                    if k < 3 or y in (1, 2):
                        add("z-", (h, x, k, y), "A", 0, cut, ranks[2])
            for n, z in enumerate(RING):
                add("y+", (h, x, z, 0), "B", cut, end, ranks[3])
                add("y-", (h, x, z, 0), "B", cut, end, ranks[3])
                link, y = ("y+", 3) if n % 2 == 0 else ("y-", 1)
                add(link, (h, x, z, y), "B", cut, end, ranks[3])
            if x == 0 and x_cols:
                for z in RING:
                    for y in (0, 3, 1, 2):
                        if (z, y) != (0, 0):
                            add("x", (h, 0, z, y), "X", cols - x_cols, cols, ranks[4])
    for number, s in enumerate(sends):
        s["id"] = number
    arrives = {(s["lands"], s["part"]): s["id"] for s in sends}
    for s in sends:
        h, x, z, y = s["unit"]
        if (x, z, y) == (0, 0, 0):
            s["needs"] = None
        elif (x, z, y) == (1, 0, 0):
            s["needs"] = arrives[s["unit"], "F"]
        else:
            s["needs"] = arrives[s["unit"], "B" if s["part"] == "X" else s["part"]]
    forwarded = {s["needs"] for s in sends}
    groups = {}
    for s in sends:
        key = (s["part"], s["lands"][:3]) if s["id"] not in forwarded else s["id"]
        groups.setdefault(key, []).append(s)
    for sem, members in enumerate(groups.values()):
        assert len({(s["lo"], s["hi"]) for s in members}) == 1
        for s in members:
            s["sem"], s["group"] = sem, len(members)
    free, landed, left = dict.fromkeys(LINKS, 0.0), {None: 0.0}, list(sends)
    when = {}; latest = dict.fromkeys(LINKS, 0.0)
    while left:
        best = None
        for s in left:
            if s["needs"] in landed:
                key = (max(landed[s["needs"]], free[s["link"]]), s["unit"][:2], s["rank"], s["id"])
                if best is None or key < best[0]:
                    best = key, s
        (start, *_), s = best
        free[s["link"]] = start + (s["hi"] - s["lo"]) * TILE
        landed[s["id"]] = free[s["link"]] + LATENCY
        early = start - AHEAD if s["part"] == "X" else 0.0
        latest[s["link"]] = max(latest[s["link"]], landed[s["needs"]], early)
        when[s["id"]] = latest[s["link"]]
        left.remove(s)
    events = [(when[s["id"]], 0, s["id"], s) for s in sends]
    batches = []
    for h in range(NH):
        for z in range(NZ):
            wanted = [arrives[(h, x, z, y), p] for x in range(NX) for y in range(NY) for p in "FABX" if ((h, x, z, y), p) in arrives]
            batches.append((max(landed[w] for w in wanted), h, z, wanted))
    batches.sort()
    return sends, events, batches, free


def timeline(schedule, lags):
    sends, events, batches, _ = schedule
    couples = [
        (two[1][0], two[0][1], (two[0][2], two[1][2]), two[0][3] + two[1][3])
        for two in zip(batches[::2], batches[1::2])
    ]
    assert all(one[1] == other[1] for one, other in zip(batches[::2], batches[1::2]))
    first = max(b[0] for b in couples if b[1] == 0)
    steps = [(first + sum(lags[: n + 1]), 2, n, None) for n in range(len(lags))]
    marked = [(b[0], 1, n, b) for n, b in enumerate(couples)]
    marked += [(PREPARE_AT + n * PREPARE_STEP, 3, n, None) for n in range(PREPARE_PARTS)]
    segments, issue, order = [], [], []
    for _, kind, n, what in sorted(events + marked + steps, key=lambda e: e[:3]):
        if kind == 1:
            segments.append((issue, what[3]))
            order.append((what[1], what[2]))
            issue = []
        else:
            issue.append(what if kind == 0 else (kind, n))
    assert not any(isinstance(e, dict) for e in issue)
    return segments, order, issue


def same(one, other):
    keys = ("link", "part", "lo", "hi")
    return all(one[k] == other[k] for k in keys)


def table(values, index):
    total = jnp.int32(0)
    for n, v in enumerate(values):
        if v:
            total = total + jnp.where(index == n, v, 0)
    return total


def em_kernel(
    sends, line, temp, whole_particles, whole_low, whole_high, templates,
    rows, temps, edge, num, weights_1, inverse, evid,
    particles, tilt_low, tilt_high, split, pairs, masks, weights_0, scores, core_parts, parts, totals, stat_a, stat_b, stat_z, stat_q, stat_w, power,
    local_sem, load_sem, tilt_sem, a_send, a_recv, send_sem, recv_sem,
    ps_send, pc_recv, px_recv, z_send, z_recv, q_send, q_recv, t_send, t_recv, l_send, l_recv,
):
    segments, batches, late = line
    dom, orient = lax.axis_index("dom"), lax.axis_index("orient")
    x0, y0, z0 = orient // (NY * NZ), (orient // NZ) % NY, orient % NZ
    q0 = x0 * NY + y0
    refs, width = temps.shape
    quarter = width // 2
    half = rows.shape[0] // NH
    share = half // ND

    def at(x, y, z):
        return {"orient": (x * NY + y) * NZ + z}

    z_peer = [at(x0, y0, (z0 + k) % NZ) for k in range(NZ)]
    q_peer = [{"orient": (q0 + k) % (NX * NY) * NZ + z0} for k in range(NX * NY)]
    d_peer = [{"dom": (dom + k) % ND} for k in range(ND)]
    target = {
        "x": q_peer[NY],
        "y+": at(x0, (y0 + 1) % NY, z0),
        "y-": at(x0, (y0 + NY - 1) % NY, z0),
        "z+": z_peer[1],
        "z-": z_peer[NZ - 1],
    }
    chip_dom = dom + 1 - 2 * (dom % 2)
    side_dom = (dom + 2) % ND
    chip_peer, side_peer = {"dom": chip_dom}, {"dom": side_dom}

    load = pltpu.make_async_copy(
        templates.at[:, :, pl.ds(pl.multiple_of(dom * quarter, quarter), quarter)],
        pairs,
        load_sem,
    )
    fetch = pltpu.make_async_copy(whole_particles, particles, local_sem)
    fetch.start()
    limits = [
        pltpu.make_async_copy(src, dst, tilt_sem.at[n])
        for n, (src, dst) in enumerate(((whole_low, tilt_low), (whole_high, tilt_high)))
    ]
    for c in limits:
        c.start()
    load.start()
    barrier = pltpu.get_barrier_semaphore()
    greeted = list(target.values()) + d_peer[1:]
    for peer in greeted:
        pl.semaphore_signal(barrier, inc=1, device_id=peer, device_id_type=MESH)

    def remote(src, dst, ssem, rsem, peer):
        return pltpu.make_async_remote_copy(
            src_ref=src, dst_ref=dst, send_sem=ssem, recv_sem=rsem,
            device_id=peer, device_id_type=MESH,
        )

    z_at = [
        ((z0 + k) % NZ % ND * 2 + (z0 + k) % NZ // ND) * BATCH for k in range(NZ)
    ]
    y_at = [(y0 + k) % NY * UNIT for k in range(NY)]
    x_at = [x0 * NY * UNIT, (1 - x0) * NY * UNIT]

    def unit_row(unit):
        h, x, z, y = unit
        return h * half + x_at[x] + z_at[z] + y_at[y]

    def relayout(i, carry):
        r = pl.ds(pl.multiple_of(i * 16, 16), 16)
        for c in range(2):
            temps[r, c * quarter : (c + 1) * quarter] = pairs[r, c, :]
        return carry

    local = particles.shape[0]
    item = lax.broadcasted_iota(jnp.int32, (local, 1), 0)
    low, high = jnp.zeros((local, 1), jnp.float32), jnp.zeros((local, 1), jnp.float32)
    for c in limits:
        c.wait()
    for n in range(local):
        low = jnp.where(item == n, tilt_low[n].astype(jnp.float32), low)
        high = jnp.where(item == n, tilt_high[n].astype(jnp.float32), high)
    column = lax.broadcasted_iota(jnp.int32, (local, quarter), 1)
    bins = (column * 37 % NBIN).astype(jnp.float32)
    seen = (low <= bins) & (bins < high)
    stash = jnp.where(column == LOW_AT, low, jnp.where(column == HIGH_AT, high, 0.0))
    fetch.wait()
    for c in range(2):
        for d in range(ND):
            piece = particles[:, c, d * quarter : (d + 1) * quarter].astype(jnp.float32)
            piece = jnp.where(seen, piece, stash if c == 0 else 0.0)
            split[d * local : (d + 1) * local, c * quarter : (c + 1) * quarter] = piece.astype(
                jnp.bfloat16
            )
    pl.semaphore_wait(barrier, len(greeted))

    own_at = unit_row((0, 0, 0, 0))

    def split_at(owner):
        return split.at[pl.ds(pl.multiple_of(owner * local, local), local)]

    def own_rows(source):
        row = own_at + source // 2 * half + source % 2 * local
        return rows.at[pl.ds(pl.multiple_of(row, local), local)]

    diag_dom = (chip_dom + 2) % ND
    others = ((chip_dom, chip_peer), (side_dom, side_peer), (diag_dom, {"dom": diag_dom}))

    def a_copy(k, source, owner):
        return remote(split_at(owner), own_rows(source), a_send.at[k], a_recv.at[k], others[k][1])

    for k in (1, 2, 0):
        a_copy(k, dom, others[k][0]).start()
    own = pltpu.make_async_copy(split_at(dom), own_rows(dom), local_sem)
    own.start()

    def copy_of(s, unit):
        columns = pl.ds(s["lo"] * LANES, (s["hi"] - s["lo"]) * LANES)
        place = rows.at[pl.ds(pl.multiple_of(unit_row(unit), UNIT), UNIT), columns]
        return remote(
            place, place, send_sem.at[unit[0]], recv_sem.at[s["sem"]], target[s["link"]]
        )

    heard = set()

    def hear(number):
        if number is None or sends[number]["sem"] in heard:
            return
        s = sends[number]
        heard.add(s["sem"])
        h, x, z, _ = s["lands"]
        columns = pl.ds(s["lo"] * LANES, (s["hi"] - s["lo"]) * LANES)
        if s["group"] == 1:
            row = unit_row(s["lands"])
        else:
            row = h * half + x_at[x] + z_at[z]
        place = rows.at[pl.ds(pl.multiple_of(row, UNIT), UNIT * s["group"]), columns]
        remote(
            place, place, send_sem.at[h], recv_sem.at[s["sem"]], target[s["link"]]
        ).wait_recv()

    def owner_of(slot):
        return slot % (2 * ND) // 2

    def core_copy(slot):
        return remote(
            scores.at[slot], core_parts.at[slot], ps_send, pc_recv.at[slot], chip_peer
        )

    def side_copy(slot):
        part = slot // (2 * ND) * 2 + slot % 2
        return remote(
            scores.at[slot], parts.at[part], ps_send, px_recv.at[part], side_peer
        )

    def combine(slot):
        @pl.when(owner_of(slot) % 2 == dom % 2)
        def _():
            core_copy(slot).wait_recv()
            scores[slot] = scores[slot] + core_parts[slot]

            @pl.when(owner_of(slot) != dom)
            def _():
                side_copy(slot).start()

    def evidence_of(peak, mass):
        return jnp.concatenate([peak, mass, peak, mass], axis=0)

    def send_stats(src, slot, peers, ssem, rsem):
        for peer in peers:
            remote(src, slot, ssem, rsem, peer).start()

    def all_but_one(slots, sem):
        most = slots.at[pl.ds(0, slots.shape[0] - 1)]
        return pltpu.make_async_copy(most, most, sem)

    def merged(both):
        peak = jnp.max(both[:, :2], axis=0)
        return peak, jnp.sum(both[:, 2:4] * jnp.exp(both[:, :2] - peak[None]), axis=0)

    def total_copy(h, n, k, owner, peer):
        ref = totals.at[h, owner, k]
        return remote(ref, ref, t_send.at[h], t_recv.at[h, n, k], peer)

    def sum_scores(h):
        peaks, masses = [], []
        for k in range(2):
            mine = h * 2 * ND + dom * 2 + k
            side_copy(mine).wait_recv()
            total = (scores[mine] + parts[h * 2 + k]) * temp
            totals[h, dom, k] = total
            peak = jnp.max(total, axis=0, keepdims=True)
            peaks.append(peak)
            masses.append(jnp.sum(jnp.exp(total - peak), axis=0, keepdims=True))
        tile = evidence_of(jnp.concatenate(peaks, axis=0), jnp.concatenate(masses, axis=0))
        stat_a[h] = tile
        stat_z[h, z0] = tile
        send_stats(stat_a.at[h], stat_z.at[h, z0], z_peer[1:], z_send.at[h], z_recv.at[h])
        total_copy(h, 0, 0, dom, side_peer).start()
        for k in range(2):
            total_copy(h, 1, k, dom, chip_peer).start()

    def merge_z(h):
        all_but_one(stat_z.at[h], z_recv.at[h]).wait()
        tile = evidence_of(*merged(stat_z[h]))
        stat_b[h] = tile
        if h == 0:
            stat_q[q0] = tile
            send_stats(stat_b.at[0], stat_q.at[q0], q_peer[1:], q_send.at[0], q_recv.at[0])
        else:
            slot = dom * NX * NY + q0
            stat_w[slot] = tile
            wide = [
                dict(q_peer[n % (NX * NY)], **d_peer[n // (NX * NY)])
                for n in range(1, ND * NX * NY)
            ]
            send_stats(stat_b.at[1], stat_w.at[slot], wide, q_send.at[1], q_recv.at[1])
        total_copy(h, 0, 1, dom, side_peer).start()

    weights = (weights_0, weights_1)

    def l_copy(k, owner):
        ref = evid.at[0, owner]
        return remote(ref, ref, l_send.at[k], l_recv.at[k], d_peer[k])

    def weigh_first():
        all_but_one(stat_q, q_recv.at[0]).wait()
        peak, mass = merged(stat_q[...])
        log_evidence = peak + jnp.log(mass)
        evid[0, dom] = evidence_of(log_evidence, mass)
        for k in range(1, ND):
            l_copy(k, dom).start()
        fill_weights(0, dom, log_evidence)

    def weigh_second():
        all_but_one(stat_w, q_recv.at[1]).wait()
        for owner in range(ND):
            peak, mass = merged(stat_w[owner * NX * NY : (owner + 1) * NX * NY])
            log_evidence = peak + jnp.log(mass)
            evid[1, owner] = evidence_of(log_evidence, mass)
            fill_weights(1, owner, log_evidence)

    def fill_weights(h, owner, log_evidence):
        for k in range(2):
            w = jnp.exp(totals[h, owner, k] - log_evidence[k : k + 1])
            place = pl.ds(pl.multiple_of(owner * share + k * BATCH, BATCH), BATCH)
            weights[h][:, place] = w.astype(jnp.bfloat16)

    def forward(h):
        for k in range(2):
            total_copy(h, 0, k, side_dom, side_peer).wait_recv()
            total_copy(h, 2, k, side_dom, chip_peer).start()

    def receive(h):
        for k in range(2):
            total_copy(h, 1, k, chip_dom, chip_peer).wait_recv()
            total_copy(h, 2, k, diag_dom, chip_peer).wait_recv()

    def fill_others():
        for k in range(1, ND):
            owner = (dom + ND - k) % ND
            l_copy(k, owner).wait_recv()
            fill_weights(0, owner, evid[0, owner][:2])

    def first_numerator(piece):
        columns = pl.ds(piece * quarter, quarter)
        num[:, columns] = jnp.dot(
            weights_0[...], rows[:half, columns], preferred_element_type=jnp.float32
        )

    last_of = [max(n for n, b in enumerate(batches) if b[0] == h) for h in range(NH)]
    assert last_of == [len(batches) // 2 - 1, len(batches) - 1]

    def combine_last(h):
        for slot in slots_of(last_of[h]):
            combine(slot)

    chain = (combine_last, sum_scores, merge_z)

    def prepare(part):
        if part == 0:
            load.wait()
        share_of = refs // 16 // PREPARE_PARTS
        lax.fori_loop(part * share_of, (part + 1) * share_of, relayout, 0)
        if part < PREPARE_PARTS - 1:
            return
        total = jnp.zeros((refs, LANES), jnp.float32)
        for c in range(width // LANES):
            piece = temps[:, c * LANES : (c + 1) * LANES].astype(jnp.float32)
            total = total + piece * piece
        total = 0.5 * total
        for c in range(3):
            head = total.astype(jnp.bfloat16)
            power[c] = head
            total = total - head.astype(jnp.float32)
        edge[...] = temps[:, :LANES]
        lane = lax.broadcasted_iota(jnp.int32, (refs, LANES), 1)
        stash = (lane == LOW_AT) | (lane == HIGH_AT)
        temps[:, :LANES] = jnp.where(
            stash, jnp.zeros((refs, LANES), jnp.bfloat16), temps[:, :LANES]
        )

    def slots_of(phase):
        bh = table([b[0] for b in batches], phase)
        slots = []
        for n in range(2):
            bz = (z0 + table([b[1][n] for b in batches], phase)) % NZ
            slots.append(bh * 2 * ND + bz % ND * 2 + bz // ND)
        return slots

    opening = [s for s in sends if s["needs"] is None]
    twins = [(s, next(t for t in opening if t["unit"][0] == 1 and same(s, t)))
             for s in opening if s["unit"][0] == 0]
    near = dom // 2
    own.wait()
    a_copy(0, chip_dom, dom).wait_recv()
    for h in (near, 1 - near):
        for s, t in twins:
            columns = pl.ds(s["lo"] * LANES, (s["hi"] - s["lo"]) * LANES)
            row = unit_row((h, 0, 0, 0))
            place = rows.at[pl.ds(pl.multiple_of(row, UNIT), UNIT), columns]
            sem = s["sem"] + h * (t["sem"] - s["sem"])
            remote(
                place, place, send_sem.at[h], recv_sem.at[sem], target[s["link"]]
            ).start()
        if h is near:
            for k in (1, 2):
                a_copy(k, others[k][0], dom).wait_recv()

    def phase_body(phase, carry):
        for n, (issue, wanted) in enumerate(segments):

            @pl.when(phase == n)
            def _(n=n, issue=issue, wanted=wanted):
                for s in issue:
                    if isinstance(s, dict) and s["needs"] is None:
                        continue
                    if isinstance(s, tuple):
                        if s[0] == 3:
                            prepare(s[1])
                        else:
                            chain[s[1]](0)
                    else:
                        hear(s["needs"])
                        copy_of(s, s["unit"]).start()
                for w in wanted:
                    hear(w)

        slots = slots_of(phase)
        heres = [pl.ds(pl.multiple_of(slot * BATCH, BATCH), BATCH) for slot in slots]
        lane = lax.broadcasted_iota(jnp.int32, (BATCH, LANES), 1)
        bins = (lane * 37 % NBIN).astype(jnp.float32)
        both = []
        for here in heres:
            lims = rows[here, :LANES].astype(jnp.float32)
            seen = (bins >= lims[:, LOW_AT : LOW_AT + 1]) & (bins < lims[:, HIGH_AT : HIGH_AT + 1])
            mask = jnp.where(seen, 1.0, 0.0).astype(jnp.bfloat16)
            masks[here, :] = mask
            both.append(mask)
        mask = jnp.concatenate(both, axis=0)
        nt = (((1,), (1,)), ((), ()))
        penalty = lax.dot_general(power[2], mask, nt, preferred_element_type=jnp.float32)
        for c in (1, 0):
            penalty = penalty + lax.dot_general(
                power[c], mask, nt, preferred_element_type=jnp.float32
            )
        batch = jnp.concatenate([rows[here, :] for here in heres], axis=0)
        corr = lax.dot_general(temps[...], batch, nt, preferred_element_type=jnp.float32)
        result = corr - penalty
        for n, slot in enumerate(slots):
            scores[slot] = result[:, n * BATCH : (n + 1) * BATCH]

            @pl.when(owner_of(slot) % 2 != dom % 2)
            def _(slot=slot):
                core_copy(slot).start()

        @pl.when((phase > 0) & (phase != last_of[0] + 1))
        def _():
            for slot in slots_of(phase - 1):
                combine(slot)

        return carry

    lax.fori_loop(0, len(segments), phase_body, 0)

    for step in late:
        chain[step[1]](0)
    combine_last(1)
    weigh_first()
    forward(0)
    sum_scores(1)
    receive(0)
    fill_others()
    first_numerator(0)
    merge_z(1)
    forward(1)
    for h in range(NH):
        sent = sum((s["hi"] - s["lo"]) * UNIT for s in sends if s["unit"][0] == h)
        assert sent * LANES % width == 0 and sent * LANES // width <= half
        every = rows.at[pl.ds(0, sent * LANES // width)]
        pltpu.make_async_copy(every, every, send_sem.at[h]).wait()
    first_numerator(1)
    receive(1)
    den = jnp.dot(weights_0[...], masks[:half], preferred_element_type=jnp.float32)
    inverse[...] = den

    for k in range(ND - 1):
        a_copy(k, dom, others[k][0]).wait_send()
    sent = scores.at[pl.ds(0, (NH * 2 * ND) * 3 // 4)]
    pltpu.make_async_copy(sent, sent, ps_send).wait()
    for h in range(NH):
        all_but_one(stat_z.at[h], z_send.at[h]).wait()
        sent = totals.at[h, pl.ds(0, 3)]
        pltpu.make_async_copy(sent, sent, t_send.at[h]).wait()
    all_but_one(stat_q, q_send.at[0]).wait()
    for k in range(1, ND):
        l_copy(k, dom).wait_send()
    weigh_second()
    den = inverse[...] + jnp.dot(weights_1[...], masks[half:], preferred_element_type=jnp.float32)
    inverse[...] = 1.0 / (den + 1.0)
    all_but_one(stat_w, q_send.at[1]).wait()


def update_kernel(weights, inverse, rows, num, temps, edge, evid, out, evid_out, staged, sems):
    refs, width = num.shape
    quarter, half = width // 2, weights.shape[1]
    tile = staged.shape[3]

    dom = lax.axis_index("dom")
    source = evid[dom // 2]
    lane = lax.broadcasted_iota(jnp.int32, (ND, LANES), 1)
    row = lax.broadcasted_iota(jnp.int32, (ND, LANES), 0)
    local = LANES // 16
    mine = (lane // (LANES // ND) == row) & (lane // local % 2 == dom % 2)
    spread = []
    for z in range(NZ):
        values = jnp.broadcast_to(source[z % ND, z // ND : z // ND + 1], (ND, LANES))
        spread.append(jnp.where(mine, values, 0.0))
    spread = jnp.concatenate(spread, axis=1)
    at = lax.broadcasted_iota(jnp.int32, (NZ * LANES, LANES), 0)
    to = lax.broadcasted_iota(jnp.int32, (NZ * LANES, LANES), 1)
    goal = at % LANES // 16 % 2 * (LANES // 2) + at // LANES * local + at % local
    place = jnp.where(goal == to, 1.0, 0.0).astype(jnp.bfloat16)
    moved_parts = []
    for _ in range(3):
        head = spread.astype(jnp.bfloat16)
        spread = spread - head.astype(jnp.float32)
        moved_parts.append(jnp.dot(head, place, preferred_element_type=jnp.float32))
    evid_out[...] = moved_parts[0] + (moved_parts[1] + moved_parts[2])

    def copy(j):
        columns = pl.ds(pl.multiple_of(j * tile, tile), tile)
        return pltpu.make_async_copy(staged.at[j % 2], out.at[:, :, columns], sems.at[j % 2])

    lane = lax.broadcasted_iota(jnp.int32, (refs, LANES), 1)
    stash = (lane == LOW_AT) | (lane == HIGH_AT)
    scale = jnp.concatenate([inverse[...]] * (tile // LANES), axis=1)

    def step(j, carry):
        @pl.when(j >= 2)
        def _():
            copy(j - 2).wait()

        for c in range(2):
            columns = pl.ds(pl.multiple_of(c * quarter + j * tile, tile), tile)
            total = num[:, columns] + jnp.dot(
                weights[...], rows[half:, columns], preferred_element_type=jnp.float32
            )
            staged[j % 2, :, c, :] = (total + temps[:, columns].astype(jnp.float32)) * scale

        @pl.when(j == 0)
        def _():
            first = staged[0, :, 0, :LANES]
            kept = edge[...].astype(jnp.float32) * inverse[...]
            staged[0, :, 0, :LANES] = jnp.where(stash, kept, first)

        copy(j).start()
        return carry

    steps = quarter // tile
    lax.fori_loop(0, steps, step, 0)
    copy(steps - 2).wait()
    copy(steps - 1).wait()


def on_device(particles, templates, tilt_low, tilt_high):
    local, _, band = particles.shape
    refs = templates.shape[0]
    quarter = band // ND
    width = 2 * quarter
    temp = 3.0 / math.sqrt(band)
    schedule = plan(width // LANES, CUTS, RANKS)
    line = timeline(schedule, LAGS)
    count = 1 + max(s["sem"] for s in schedule[0])
    total = NX * NY * NZ * ND * local
    half = total // NH
    bf16, f32 = jnp.bfloat16, jnp.float32
    dma = pltpu.SemaphoreType.DMA
    vmem = pl.BlockSpec(memory_space=pltpu.VMEM)
    rows, temps, edge, num, weights, inverse, evidence = pl.pallas_call(
        functools.partial(em_kernel, schedule[0], line, temp),
        out_shape=(
            jax.ShapeDtypeStruct((total, width), bf16),
            jax.ShapeDtypeStruct((refs, width), bf16),
            jax.ShapeDtypeStruct((refs, LANES), bf16),
            jax.ShapeDtypeStruct((refs, width), f32),
            jax.ShapeDtypeStruct((refs, half), bf16),
            jax.ShapeDtypeStruct((refs, LANES), f32),
            jax.ShapeDtypeStruct((NH, ND, 8, LANES), f32),
        ),
        in_specs=[pl.BlockSpec(memory_space=pltpu.HBM)] * 4,
        out_specs=(vmem,) * 7,
        scratch_shapes=[
            pltpu.VMEM(particles.shape, bf16),
            pltpu.SMEM((local,), jnp.int32),
            pltpu.SMEM((local,), jnp.int32),
            pltpu.VMEM((ND * local, width), bf16),
            pltpu.VMEM((refs, 2, quarter), bf16),
            pltpu.VMEM((total, LANES), bf16),
            pltpu.VMEM((refs, half), bf16),
            pltpu.VMEM((NH * 2 * ND, refs, LANES), f32),
            pltpu.VMEM((NH * 2 * ND, refs, LANES), f32),
            pltpu.VMEM((NH * 2, refs, LANES), f32),
            pltpu.VMEM((NH, ND, 2, refs, LANES), f32),
            pltpu.VMEM((NH, 8, LANES), f32),
            pltpu.VMEM((NH, 8, LANES), f32),
            pltpu.VMEM((NH, NZ, 8, LANES), f32),
            pltpu.VMEM((NX * NY, 8, LANES), f32),
            pltpu.VMEM((ND * NX * NY, 8, LANES), f32),
            pltpu.VMEM((3, refs, LANES), bf16),
            dma(()),
            dma(()),
            dma((2,)),
            dma((ND - 1,)),
            dma((ND - 1,)),
            dma((NH,)),
            dma((count,)),
            dma(()),
            dma((NH * 2 * ND,)),
            dma((NH * 2,)),
            dma((NH,)),
            dma((NH,)),
            dma((NH,)),
            dma((NH,)),
            dma((NH,)),
            dma((NH, 3, 2)),
            dma((ND,)),
            dma((ND,)),
        ],
        compiler_params=pltpu.CompilerParams(
            collective_id=0, has_side_effects=True, vmem_limit_bytes=18 * 1024 * 1024
        ),
    )(
        *(
            pltpu.with_memory_space_constraint(a, pltpu.HBM)
            for a in (particles, tilt_low, tilt_high, templates)
        )
    )
    tile = 1024
    updated, evidence = pl.pallas_call(
        update_kernel,
        out_shape=(
            jax.ShapeDtypeStruct((refs, 2, quarter), f32),
            jax.ShapeDtypeStruct((ND, LANES), f32),
        ),
        in_specs=[vmem] * 7,
        out_specs=(pl.BlockSpec(memory_space=pltpu.HBM), vmem),
        scratch_shapes=[pltpu.VMEM((2, refs, 2, tile), f32), dma((2,))],
        compiler_params=pltpu.CompilerParams(vmem_limit_bytes=12 * 1024 * 1024),
    )(weights, inverse, rows, num, temps, edge, evidence)
    return updated, evidence.reshape(-1)


def solution(mesh):
    in_specs = (
        P(("dom", "orient"), None, None),
        P("orient", None, None),
        P(("dom", "orient")),
        P(("dom", "orient")),
    )
    out_specs = (P("orient", None, "dom"), P("dom"))
    return jax.shard_map(
        on_device, mesh=mesh, in_specs=in_specs, out_specs=out_specs, check_vma=False
    )
```

```python
import functools
import math

import jax
import jax.numpy as jnp
from jax import lax
from jax.experimental import pallas as pl
from jax.experimental.pallas import tpu as pltpu
from jax.sharding import PartitionSpec as P

NBIN = 64
NX, NY, NZ, ND, NH = 2, 4, 8, 4, 2
LANES = 128
RING = (0, 7, 1, 6, 2, 5, 3, 4)
LINKS = ("x", "y+", "y-", "z+", "z-")
LATENCY = 4.25
TILE = 0.0879
AHEAD = 2.0
CUTS = ((13, 9, 11), (13, 8, 10))
RANKS = (3, 0, 2, 3, 0)
LAGS = (2.5, 11.0, 9.0)
PREPARE_AT, PREPARE_STEP, PREPARE_PARTS = 6.0, 3.0, 8
BATCH = 128
UNIT = 16
LOW_AT, HIGH_AT = 19, 83
MESH = pl.DeviceIdType.MESH


def moved(unit, link):
    h, x, z, y = unit
    if link == "x":
        return h, 1 - x, z, y
    step = -1 if link[1] == "+" else 1
    return (h, x, (z + step) % NZ, y) if link[0] == "z" else (h, x, z, (y + step) % NY)

def plan(cols, cuts, ranks=(0, 1, 2, 2, 3)):
    sends = []
    def add(link, unit, part, lo, hi, rank):
        sends.append(dict(link=link, unit=unit, part=part, lo=lo, hi=hi, rank=rank, lands=moved(unit, link)))
    for h in range(NH):
        first_a, second_a, x_cols = cuts[h]
        add("x", (h, 0, 0, 0), "F", 0, cols, 0)
        for x in (0, 1):
            cut, end = (first_a, cols) if x == 0 else (second_a, cols - x_cols)
            plus = (x + h) % 2 == 0
            add("y+", (h, x, 0, 0), "A", 0, cut, ranks[0])
            add("y-", (h, x, 0, 0), "A", 0, cut, ranks[0])
            link, y = ("y+", 3) if plus else ("y-", 1)
            add(link, (h, x, 0, y), "A", 0, cut, ranks[0])
            for k in range(4):
                if k < 3 or plus:
                    add("z+", (h, x, -k % NZ, 0), "B", cut, end, ranks[1])
                if k < 3 or not plus:
                    add("z-", (h, x, k, 0), "B", cut, end, ranks[1])
            for k in range(4):
                for y in (0, 3, 1, 2):
                    if k < 3 or y in (0, 3):
                        add("z+", (h, x, -k % NZ, y), "A", 0, cut, ranks[2])
                    if k < 3 or y in (1, 2):
                        add("z-", (h, x, k, y), "A", 0, cut, ranks[2])
            for n, z in enumerate(RING):
                add("y+", (h, x, z, 0), "B", cut, end, ranks[3])
                add("y-", (h, x, z, 0), "B", cut, end, ranks[3])
                link, y = ("y+", 3) if n % 2 == 0 else ("y-", 1)
                add(link, (h, x, z, y), "B", cut, end, ranks[3])
            if x == 0 and x_cols:
                for z in RING:
                    for y in (0, 3, 1, 2):
                        if (z, y) != (0, 0):
                            add("x", (h, 0, z, y), "X", cols - x_cols, cols, ranks[4])
    for number, s in enumerate(sends):
        s["id"] = number
    arrives = {(s["lands"], s["part"]): s["id"] for s in sends}
    for s in sends:
        h, x, z, y = s["unit"]
        if (x, z, y) == (0, 0, 0):
            s["needs"] = None
        elif (x, z, y) == (1, 0, 0):
            s["needs"] = arrives[s["unit"], "F"]
        else:
            s["needs"] = arrives[s["unit"], "B" if s["part"] == "X" else s["part"]]
    forwarded = {s["needs"] for s in sends}
    groups = {}
    for s in sends:
        key = (s["part"], s["lands"][:3]) if s["id"] not in forwarded else s["id"]
        groups.setdefault(key, []).append(s)
    for sem, members in enumerate(groups.values()):
        assert len({(s["lo"], s["hi"]) for s in members}) == 1
        for s in members:
            s["sem"], s["group"] = sem, len(members)
    free, landed, left = dict.fromkeys(LINKS, 0.0), {None: 0.0}, list(sends)
    when = {}; latest = dict.fromkeys(LINKS, 0.0)
    while left:
        best = None
        for s in left:
            if s["needs"] in landed:
                key = (max(landed[s["needs"]], free[s["link"]]), s["unit"][:2], s["rank"], s["id"])
                if best is None or key < best[0]:
                    best = key, s
        (start, *_), s = best
        free[s["link"]] = start + (s["hi"] - s["lo"]) * TILE
        landed[s["id"]] = free[s["link"]] + LATENCY
        early = start - AHEAD if s["part"] == "X" else 0.0
        latest[s["link"]] = max(latest[s["link"]], landed[s["needs"]], early)
        when[s["id"]] = latest[s["link"]]
        left.remove(s)
    events = [(when[s["id"]], 0, s["id"], s) for s in sends]
    batches = []
    for h in range(NH):
        for z in range(NZ):
            wanted = [arrives[(h, x, z, y), p] for x in range(NX) for y in range(NY) for p in "FABX" if ((h, x, z, y), p) in arrives]
            batches.append((max(landed[w] for w in wanted), h, z, wanted))
    batches.sort()
    return sends, events, batches, free


def timeline(schedule, lags):
    sends, events, batches, _ = schedule
    couples = [
        (two[1][0], two[0][1], (two[0][2], two[1][2]), two[0][3] + two[1][3])
        for two in zip(batches[::2], batches[1::2])
    ]
    assert all(one[1] == other[1] for one, other in zip(batches[::2], batches[1::2]))
    first = max(b[0] for b in couples if b[1] == 0)
    steps = [(first + sum(lags[: n + 1]), 2, n, None) for n in range(len(lags))]
    marked = [(b[0], 1, n, b) for n, b in enumerate(couples)]
    marked += [(PREPARE_AT + n * PREPARE_STEP, 3, n, None) for n in range(PREPARE_PARTS)]
    segments, issue, order = [], [], []
    for _, kind, n, what in sorted(events + marked + steps, key=lambda e: e[:3]):
        if kind == 1:
            segments.append((issue, what[3]))
            order.append((what[1], what[2]))
            issue = []
        else:
            issue.append(what if kind == 0 else (kind, n))
    assert not any(isinstance(e, dict) for e in issue)
    return segments, order, issue


def same(one, other):
    keys = ("link", "part", "lo", "hi")
    return all(one[k] == other[k] for k in keys)


def table(values, index):
    total = jnp.int32(0)
    for n, v in enumerate(values):
        if v:
            total = total + jnp.where(index == n, v, 0)
    return total


def em_kernel(
    sends, line, temp, whole_particles, whole_low, whole_high, templates,
    rows, temps, edge, num, weights_1, inverse, evid,
    particles, tilt_low, tilt_high, split, pairs, masks, weights_0, scores, core_parts, parts, totals, stat_a, stat_b, stat_z, stat_q, stat_w, power,
    local_sem, load_sem, tilt_sem, a_send, a_recv, send_sem, recv_sem,
    ps_send, pc_recv, px_recv, z_send, z_recv, q_send, q_recv, t_send, t_recv, l_send, l_recv,
):
    segments, batches, late = line
    dom, orient = lax.axis_index("dom"), lax.axis_index("orient")
    x0, y0, z0 = orient // (NY * NZ), (orient // NZ) % NY, orient % NZ
    q0 = x0 * NY + y0
    refs, width = temps.shape
    quarter = width // 2
    half = rows.shape[0] // NH
    share = half // ND

    def at(x, y, z):
        return {"orient": (x * NY + y) * NZ + z}

    z_peer = [at(x0, y0, (z0 + k) % NZ) for k in range(NZ)]
    q_peer = [{"orient": (q0 + k) % (NX * NY) * NZ + z0} for k in range(NX * NY)]
    d_peer = [{"dom": (dom + k) % ND} for k in range(ND)]
    target = {
        "x": q_peer[NY],
        "y+": at(x0, (y0 + 1) % NY, z0),
        "y-": at(x0, (y0 + NY - 1) % NY, z0),
        "z+": z_peer[1],
        "z-": z_peer[NZ - 1],
    }
    chip_dom = dom + 1 - 2 * (dom % 2)
    side_dom = (dom + 2) % ND
    chip_peer, side_peer = {"dom": chip_dom}, {"dom": side_dom}

    load = pltpu.make_async_copy(
        templates.at[:, :, pl.ds(pl.multiple_of(dom * quarter, quarter), quarter)],
        pairs,
        load_sem,
    )
    fetch = pltpu.make_async_copy(whole_particles, particles, local_sem)
    fetch.start()
    limits = [
        pltpu.make_async_copy(src, dst, tilt_sem.at[n])
        for n, (src, dst) in enumerate(((whole_low, tilt_low), (whole_high, tilt_high)))
    ]
    for c in limits:
        c.start()
    load.start()
    barrier = pltpu.get_barrier_semaphore()
    greeted = list(target.values()) + d_peer[1:]
    for peer in greeted:
        pl.semaphore_signal(barrier, inc=1, device_id=peer, device_id_type=MESH)

    def remote(src, dst, ssem, rsem, peer):
        return pltpu.make_async_remote_copy(
            src_ref=src, dst_ref=dst, send_sem=ssem, recv_sem=rsem,
            device_id=peer, device_id_type=MESH,
        )

    z_at = [
        ((z0 + k) % NZ % ND * 2 + (z0 + k) % NZ // ND) * BATCH for k in range(NZ)
    ]
    y_at = [(y0 + k) % NY * UNIT for k in range(NY)]
    x_at = [x0 * NY * UNIT, (1 - x0) * NY * UNIT]

    def unit_row(unit):
        h, x, z, y = unit
        return h * half + x_at[x] + z_at[z] + y_at[y]

    def relayout(i, carry):
        r = pl.ds(pl.multiple_of(i * 16, 16), 16)
        for c in range(2):
            temps[r, c * quarter : (c + 1) * quarter] = pairs[r, c, :]
        return carry

    local = particles.shape[0]
    item = lax.broadcasted_iota(jnp.int32, (local, 1), 0)
    low, high = jnp.zeros((local, 1), jnp.float32), jnp.zeros((local, 1), jnp.float32)
    for c in limits:
        c.wait()
    for n in range(local):
        low = jnp.where(item == n, tilt_low[n].astype(jnp.float32), low)
        high = jnp.where(item == n, tilt_high[n].astype(jnp.float32), high)
    column = lax.broadcasted_iota(jnp.int32, (local, quarter), 1)
    bins = (column * 37 % NBIN).astype(jnp.float32)
    seen = (low <= bins) & (bins < high)
    stash = jnp.where(column == LOW_AT, low, jnp.where(column == HIGH_AT, high, 0.0))
    fetch.wait()
    for c in range(2):
        for d in range(ND):
            piece = particles[:, c, d * quarter : (d + 1) * quarter].astype(jnp.float32)
            piece = jnp.where(seen, piece, stash if c == 0 else 0.0)
            split[d * local : (d + 1) * local, c * quarter : (c + 1) * quarter] = piece.astype(
                jnp.bfloat16
            )
    pl.semaphore_wait(barrier, len(greeted))

    own_at = unit_row((0, 0, 0, 0))

    def split_at(owner):
        return split.at[pl.ds(pl.multiple_of(owner * local, local), local)]

    def own_rows(source):
        row = own_at + source // 2 * half + source % 2 * local
        return rows.at[pl.ds(pl.multiple_of(row, local), local)]

    diag_dom = (chip_dom + 2) % ND
    others = ((chip_dom, chip_peer), (side_dom, side_peer), (diag_dom, {"dom": diag_dom}))

    def a_copy(k, source, owner):
        return remote(split_at(owner), own_rows(source), a_send.at[k], a_recv.at[k], others[k][1])

    for k in (1, 2, 0):
        a_copy(k, dom, others[k][0]).start()
    own = pltpu.make_async_copy(split_at(dom), own_rows(dom), local_sem)
    own.start()

    def copy_of(s, unit):
        columns = pl.ds(s["lo"] * LANES, (s["hi"] - s["lo"]) * LANES)
        place = rows.at[pl.ds(pl.multiple_of(unit_row(unit), UNIT), UNIT), columns]
        return remote(
            place, place, send_sem.at[unit[0]], recv_sem.at[s["sem"]], target[s["link"]]
        )

    heard = set()

    def hear(number):
        if number is None or sends[number]["sem"] in heard:
            return
        s = sends[number]
        heard.add(s["sem"])
        h, x, z, _ = s["lands"]
        columns = pl.ds(s["lo"] * LANES, (s["hi"] - s["lo"]) * LANES)
        if s["group"] == 1:
            row = unit_row(s["lands"])
        else:
            row = h * half + x_at[x] + z_at[z]
        place = rows.at[pl.ds(pl.multiple_of(row, UNIT), UNIT * s["group"]), columns]
        remote(
            place, place, send_sem.at[h], recv_sem.at[s["sem"]], target[s["link"]]
        ).wait_recv()

    def owner_of(slot):
        return slot % (2 * ND) // 2

    def core_copy(slot):
        return remote(
            scores.at[slot], core_parts.at[slot], ps_send, pc_recv.at[slot], chip_peer
        )

    def side_copy(slot):
        part = slot // (2 * ND) * 2 + slot % 2
        return remote(
            scores.at[slot], parts.at[part], ps_send, px_recv.at[part], side_peer
        )

    def combine(slot):
        @pl.when(owner_of(slot) % 2 == dom % 2)
        def _():
            core_copy(slot).wait_recv()
            scores[slot] = scores[slot] + core_parts[slot]

            @pl.when(owner_of(slot) != dom)
            def _():
                side_copy(slot).start()

    def evidence_of(peak, mass):
        return jnp.concatenate([peak, mass, peak, mass], axis=0)

    def send_stats(src, slot, peers, ssem, rsem):
        for peer in peers:
            remote(src, slot, ssem, rsem, peer).start()

    def all_but_one(slots, sem):
        most = slots.at[pl.ds(0, slots.shape[0] - 1)]
        return pltpu.make_async_copy(most, most, sem)

    def merged(both):
        peak = jnp.max(both[:, :2], axis=0)
        return peak, jnp.sum(both[:, 2:4] * jnp.exp(both[:, :2] - peak[None]), axis=0)

    def total_copy(h, n, k, owner, peer):
        ref = totals.at[h, owner, k]
        return remote(ref, ref, t_send.at[h], t_recv.at[h, n, k], peer)

    def sum_scores(h):
        peaks, masses = [], []
        for k in range(2):
            mine = h * 2 * ND + dom * 2 + k
            side_copy(mine).wait_recv()
            total = (scores[mine] + parts[h * 2 + k]) * temp
            totals[h, dom, k] = total
            peak = jnp.max(total, axis=0, keepdims=True)
            peaks.append(peak)
            masses.append(jnp.sum(jnp.exp(total - peak), axis=0, keepdims=True))
        tile = evidence_of(jnp.concatenate(peaks, axis=0), jnp.concatenate(masses, axis=0))
        stat_a[h] = tile
        stat_z[h, z0] = tile
        send_stats(stat_a.at[h], stat_z.at[h, z0], z_peer[1:], z_send.at[h], z_recv.at[h])
        for k in range(2):
            total_copy(h, 0, k, dom, side_peer).start()
            total_copy(h, 1, k, dom, chip_peer).start()

    def merge_z(h):
        all_but_one(stat_z.at[h], z_recv.at[h]).wait()
        tile = evidence_of(*merged(stat_z[h]))
        stat_b[h] = tile
        if h == 0:
            stat_q[q0] = tile
            send_stats(stat_b.at[0], stat_q.at[q0], q_peer[1:], q_send.at[0], q_recv.at[0])
        else:
            slot = dom * NX * NY + q0
            stat_w[slot] = tile
            wide = [
                dict(q_peer[n % (NX * NY)], **d_peer[n // (NX * NY)])
                for n in range(1, ND * NX * NY)
            ]
            send_stats(stat_b.at[1], stat_w.at[slot], wide, q_send.at[1], q_recv.at[1])

    weights = (weights_0, weights_1)

    def l_copy(k, owner):
        ref = evid.at[0, owner]
        return remote(ref, ref, l_send.at[k], l_recv.at[k], d_peer[k])

    def weigh_first():
        all_but_one(stat_q, q_recv.at[0]).wait()
        peak, mass = merged(stat_q[...])
        log_evidence = peak + jnp.log(mass)
        evid[0, dom] = evidence_of(log_evidence, mass)
        for k in range(1, ND):
            l_copy(k, dom).start()
        fill_weights(0, dom, log_evidence)

    def weigh_second():
        all_but_one(stat_w, q_recv.at[1]).wait()
        for owner in range(ND):
            peak, mass = merged(stat_w[owner * NX * NY : (owner + 1) * NX * NY])
            log_evidence = peak + jnp.log(mass)
            evid[1, owner] = evidence_of(log_evidence, mass)
            fill_weights(1, owner, log_evidence)

    def fill_weights(h, owner, log_evidence):
        for k in range(2):
            w = jnp.exp(totals[h, owner, k] - log_evidence[k : k + 1])
            place = pl.ds(pl.multiple_of(owner * share + k * BATCH, BATCH), BATCH)
            weights[h][:, place] = w.astype(jnp.bfloat16)

    def forward(h):
        for k in range(2):
            total_copy(h, 0, k, side_dom, side_peer).wait_recv()
            total_copy(h, 2, k, side_dom, chip_peer).start()

    def receive(h):
        for k in range(2):
            total_copy(h, 1, k, chip_dom, chip_peer).wait_recv()
            total_copy(h, 2, k, diag_dom, chip_peer).wait_recv()

    def fill_others():
        for k in range(1, ND):
            owner = (dom + ND - k) % ND
            l_copy(k, owner).wait_recv()
            fill_weights(0, owner, evid[0, owner][:2])

    def first_numerator(piece):
        columns = pl.ds(piece * quarter, quarter)
        num[:, columns] = jnp.dot(
            weights_0[...], rows[:half, columns], preferred_element_type=jnp.float32
        )

    last_of = [max(n for n, b in enumerate(batches) if b[0] == h) for h in range(NH)]
    assert last_of == [len(batches) // 2 - 1, len(batches) - 1]

    def combine_last(h):
        for slot in slots_of(last_of[h]):
            combine(slot)

    chain = (combine_last, sum_scores, merge_z)

    def prepare(part):
        if part == 0:
            load.wait()
        share_of = refs // 16 // PREPARE_PARTS
        lax.fori_loop(part * share_of, (part + 1) * share_of, relayout, 0)
        if part < PREPARE_PARTS - 1:
            return
        total = jnp.zeros((refs, LANES), jnp.float32)
        for c in range(width // LANES):
            piece = temps[:, c * LANES : (c + 1) * LANES].astype(jnp.float32)
            total = total + piece * piece
        total = 0.5 * total
        for c in range(3):
            head = total.astype(jnp.bfloat16)
            power[c] = head
            total = total - head.astype(jnp.float32)
        edge[...] = temps[:, :LANES]
        lane = lax.broadcasted_iota(jnp.int32, (refs, LANES), 1)
        stash = (lane == LOW_AT) | (lane == HIGH_AT)
        temps[:, :LANES] = jnp.where(
            stash, jnp.zeros((refs, LANES), jnp.bfloat16), temps[:, :LANES]
        )

    def slots_of(phase):
        bh = table([b[0] for b in batches], phase)
        slots = []
        for n in range(2):
            bz = (z0 + table([b[1][n] for b in batches], phase)) % NZ
            slots.append(bh * 2 * ND + bz % ND * 2 + bz // ND)
        return slots

    opening = [s for s in sends if s["needs"] is None]
    twins = [(s, next(t for t in opening if t["unit"][0] == 1 and same(s, t)))
             for s in opening if s["unit"][0] == 0]
    near = dom // 2
    own.wait()
    a_copy(0, chip_dom, dom).wait_recv()
    for h in (near, 1 - near):
        for s, t in twins:
            columns = pl.ds(s["lo"] * LANES, (s["hi"] - s["lo"]) * LANES)
            row = unit_row((h, 0, 0, 0))
            place = rows.at[pl.ds(pl.multiple_of(row, UNIT), UNIT), columns]
            sem = s["sem"] + h * (t["sem"] - s["sem"])
            remote(
                place, place, send_sem.at[h], recv_sem.at[sem], target[s["link"]]
            ).start()
        if h is near:
            for k in (1, 2):
                a_copy(k, others[k][0], dom).wait_recv()

    def phase_body(phase, carry):
        for n, (issue, wanted) in enumerate(segments):

            @pl.when(phase == n)
            def _(n=n, issue=issue, wanted=wanted):
                for s in issue:
                    if isinstance(s, dict) and s["needs"] is None:
                        continue
                    if isinstance(s, tuple):
                        if s[0] == 3:
                            prepare(s[1])
                        else:
                            chain[s[1]](0)
                    else:
                        hear(s["needs"])
                        copy_of(s, s["unit"]).start()
                for w in wanted:
                    hear(w)

        @pl.when((phase > 0) & (phase != last_of[0] + 1))
        def _():
            for slot in slots_of(phase - 1):
                combine(slot)

        slots = slots_of(phase)
        heres = [pl.ds(pl.multiple_of(slot * BATCH, BATCH), BATCH) for slot in slots]
        lane = lax.broadcasted_iota(jnp.int32, (BATCH, LANES), 1)
        bins = (lane * 37 % NBIN).astype(jnp.float32)
        both = []
        for here in heres:
            lims = rows[here, :LANES].astype(jnp.float32)
            seen = (bins >= lims[:, LOW_AT : LOW_AT + 1]) & (bins < lims[:, HIGH_AT : HIGH_AT + 1])
            mask = jnp.where(seen, 1.0, 0.0).astype(jnp.bfloat16)
            masks[here, :] = mask
            both.append(mask)
        mask = jnp.concatenate(both, axis=0)
        nt = (((1,), (1,)), ((), ()))
        penalty = lax.dot_general(power[2], mask, nt, preferred_element_type=jnp.float32)
        for c in (1, 0):
            penalty = penalty + lax.dot_general(
                power[c], mask, nt, preferred_element_type=jnp.float32
            )
        batch = jnp.concatenate([rows[here, :] for here in heres], axis=0)
        corr = lax.dot_general(temps[...], batch, nt, preferred_element_type=jnp.float32)
        result = corr - penalty
        for n, slot in enumerate(slots):
            scores[slot] = result[:, n * BATCH : (n + 1) * BATCH]

            @pl.when(owner_of(slot) % 2 != dom % 2)
            def _(slot=slot):
                core_copy(slot).start()

        return carry

    lax.fori_loop(0, len(segments), phase_body, 0)

    for step in late:
        chain[step[1]](0)
    combine_last(1)
    weigh_first()
    forward(0)
    sum_scores(1)
    receive(0)
    fill_others()
    first_numerator(0)
    merge_z(1)
    forward(1)
    for h in range(NH):
        sent = sum((s["hi"] - s["lo"]) * UNIT for s in sends if s["unit"][0] == h)
        assert sent * LANES % width == 0 and sent * LANES // width <= half
        every = rows.at[pl.ds(0, sent * LANES // width)]
        pltpu.make_async_copy(every, every, send_sem.at[h]).wait()
    first_numerator(1)
    receive(1)
    den = jnp.dot(weights_0[...], masks[:half], preferred_element_type=jnp.float32)
    inverse[...] = den

    for k in range(ND - 1):
        a_copy(k, dom, others[k][0]).wait_send()
    sent = scores.at[pl.ds(0, (NH * 2 * ND) * 3 // 4)]
    pltpu.make_async_copy(sent, sent, ps_send).wait()
    for h in range(NH):
        all_but_one(stat_z.at[h], z_send.at[h]).wait()
        sent = totals.at[h, pl.ds(0, 3)]
        pltpu.make_async_copy(sent, sent, t_send.at[h]).wait()
    all_but_one(stat_q, q_send.at[0]).wait()
    for k in range(1, ND):
        l_copy(k, dom).wait_send()
    weigh_second()
    den = inverse[...] + jnp.dot(weights_1[...], masks[half:], preferred_element_type=jnp.float32)
    inverse[...] = 1.0 / (den + 1.0)
    all_but_one(stat_w, q_send.at[1]).wait()


def update_kernel(weights, inverse, rows, num, temps, edge, evid, out, evid_out, staged, sems):
    refs, width = num.shape
    quarter, half = width // 2, weights.shape[1]
    tile = staged.shape[3]

    def copy(j):
        columns = pl.ds(pl.multiple_of(j * tile, tile), tile)
        return pltpu.make_async_copy(staged.at[j % 2], out.at[:, :, columns], sems.at[j % 2])

    lane = lax.broadcasted_iota(jnp.int32, (refs, LANES), 1)
    stash = (lane == LOW_AT) | (lane == HIGH_AT)
    scale = jnp.concatenate([inverse[...]] * (tile // LANES), axis=1)

    def step(j, carry):
        @pl.when(j >= 2)
        def _():
            copy(j - 2).wait()

        for c in range(2):
            columns = pl.ds(pl.multiple_of(c * quarter + j * tile, tile), tile)
            total = num[:, columns] + jnp.dot(
                weights[...], rows[half:, columns], preferred_element_type=jnp.float32
            )
            staged[j % 2, :, c, :] = (total + temps[:, columns].astype(jnp.float32)) * scale

        @pl.when(j == 0)
        def _():
            first = staged[0, :, 0, :LANES]
            kept = edge[...].astype(jnp.float32) * inverse[...]
            staged[0, :, 0, :LANES] = jnp.where(stash, kept, first)

        copy(j).start()
        return carry

    steps = quarter // tile
    lax.fori_loop(0, steps, step, 0)

    dom = lax.axis_index("dom")
    source = evid[dom // 2]
    lanes = lax.broadcasted_iota(jnp.int32, (ND, LANES), 1)
    row = lax.broadcasted_iota(jnp.int32, (ND, LANES), 0)
    local = LANES // 16
    mine = (lanes // (LANES // ND) == row) & (lanes // local % 2 == dom % 2)
    spread = []
    for z in range(NZ):
        values = jnp.broadcast_to(source[z % ND, z // ND : z // ND + 1], (ND, LANES))
        spread.append(jnp.where(mine, values, 0.0))
    spread = jnp.concatenate(spread, axis=1)
    at = lax.broadcasted_iota(jnp.int32, (NZ * LANES, LANES), 0)
    to = lax.broadcasted_iota(jnp.int32, (NZ * LANES, LANES), 1)
    goal = at % LANES // 16 % 2 * (LANES // 2) + at // LANES * local + at % local
    place = jnp.where(goal == to, 1.0, 0.0).astype(jnp.bfloat16)
    moved_parts = []
    for _ in range(3):
        head = spread.astype(jnp.bfloat16)
        spread = spread - head.astype(jnp.float32)
        moved_parts.append(jnp.dot(head, place, preferred_element_type=jnp.float32))
    evid_out[...] = moved_parts[0] + (moved_parts[1] + moved_parts[2])
    copy(steps - 2).wait()
    copy(steps - 1).wait()


def on_device(particles, templates, tilt_low, tilt_high):
    local, _, band = particles.shape
    refs = templates.shape[0]
    quarter = band // ND
    width = 2 * quarter
    temp = 3.0 / math.sqrt(band)
    schedule = plan(width // LANES, CUTS, RANKS)
    line = timeline(schedule, LAGS)
    count = 1 + max(s["sem"] for s in schedule[0])
    total = NX * NY * NZ * ND * local
    half = total // NH
    bf16, f32 = jnp.bfloat16, jnp.float32
    dma = pltpu.SemaphoreType.DMA
    vmem = pl.BlockSpec(memory_space=pltpu.VMEM)
    rows, temps, edge, num, weights, inverse, evidence = pl.pallas_call(
        functools.partial(em_kernel, schedule[0], line, temp),
        out_shape=(
            jax.ShapeDtypeStruct((total, width), bf16),
            jax.ShapeDtypeStruct((refs, width), bf16),
            jax.ShapeDtypeStruct((refs, LANES), bf16),
            jax.ShapeDtypeStruct((refs, width), f32),
            jax.ShapeDtypeStruct((refs, half), bf16),
            jax.ShapeDtypeStruct((refs, LANES), f32),
            jax.ShapeDtypeStruct((NH, ND, 8, LANES), f32),
        ),
        in_specs=[pl.BlockSpec(memory_space=pltpu.HBM)] * 4,
        out_specs=(vmem,) * 7,
        scratch_shapes=[
            pltpu.VMEM(particles.shape, bf16),
            pltpu.SMEM((local,), jnp.int32),
            pltpu.SMEM((local,), jnp.int32),
            pltpu.VMEM((ND * local, width), bf16),
            pltpu.VMEM((refs, 2, quarter), bf16),
            pltpu.VMEM((total, LANES), bf16),
            pltpu.VMEM((refs, half), bf16),
            pltpu.VMEM((NH * 2 * ND, refs, LANES), f32),
            pltpu.VMEM((NH * 2 * ND, refs, LANES), f32),
            pltpu.VMEM((NH * 2, refs, LANES), f32),
            pltpu.VMEM((NH, ND, 2, refs, LANES), f32),
            pltpu.VMEM((NH, 8, LANES), f32),
            pltpu.VMEM((NH, 8, LANES), f32),
            pltpu.VMEM((NH, NZ, 8, LANES), f32),
            pltpu.VMEM((NX * NY, 8, LANES), f32),
            pltpu.VMEM((ND * NX * NY, 8, LANES), f32),
            pltpu.VMEM((3, refs, LANES), bf16),
            dma(()),
            dma(()),
            dma((2,)),
            dma((ND - 1,)),
            dma((ND - 1,)),
            dma((NH,)),
            dma((count,)),
            dma(()),
            dma((NH * 2 * ND,)),
            dma((NH * 2,)),
            dma((NH,)),
            dma((NH,)),
            dma((NH,)),
            dma((NH,)),
            dma((NH,)),
            dma((NH, 3, 2)),
            dma((ND,)),
            dma((ND,)),
        ],
        compiler_params=pltpu.CompilerParams(
            collective_id=0, has_side_effects=True, vmem_limit_bytes=18 * 1024 * 1024
        ),
    )(
        *(
            pltpu.with_memory_space_constraint(a, pltpu.HBM)
            for a in (particles, tilt_low, tilt_high, templates)
        )
    )
    tile = 1024
    updated, evidence = pl.pallas_call(
        update_kernel,
        out_shape=(
            jax.ShapeDtypeStruct((refs, 2, quarter), f32),
            jax.ShapeDtypeStruct((ND, LANES), f32),
        ),
        in_specs=[vmem] * 7,
        out_specs=(pl.BlockSpec(memory_space=pltpu.HBM), vmem),
        scratch_shapes=[pltpu.VMEM((2, refs, 2, tile), f32), dma((2,))],
        compiler_params=pltpu.CompilerParams(vmem_limit_bytes=12 * 1024 * 1024),
    )(weights, inverse, rows, num, temps, edge, evidence)
    return updated, evidence.reshape(-1)


def solution(mesh):
    in_specs = (
        P(("dom", "orient"), None, None),
        P("orient", None, None),
        P(("dom", "orient")),
        P(("dom", "orient")),
    )
    out_specs = (P("orient", None, "dom"), P("dom"))
    return jax.shard_map(
        on_device, mesh=mesh, in_specs=in_specs, out_specs=out_specs, check_vma=False
    )
```
